32 devices in a mesh: dp: 8 (over z, y), tensor: 4 (over x, core).
Axes of the slice: x: 2, y: 2, z: 4, core: 2. Of those that a mesh axis runs over, the one named last changes fastest.
Arguments:
- inputs: float32 [1024, 16, 512], P('tensor', 'dp'), may hold values from -6 to 6
- qkv_weight: bfloat16 [3, 512, 512], P(None, 'dp', 'tensor'), may hold values from -0.375 to 0.375
- out_weight: bfloat16 [512, 512], P('tensor', 'dp'), may hold values from -1 to 1
- up_weight: bfloat16 [512, 2048], P('dp', 'tensor'), may hold values from -0.25 to 0.25
- down_weight: bfloat16 [2048, 512], P('tensor', 'dp'), may hold values from -0.125 to 0.125
- gain_one: float32 [512], replicated, may hold values from 0.1 to 1.9
- shift_one: float32 [512], replicated, may hold values from -1.5 to 1.5
- gain_two: float32 [512], replicated, may hold values from 0.1 to 1.9
- shift_two: float32 [512], replicated, may hold values from -1.5 to 1.5
- lengths: int32 [16], P('dp'), may hold values from 512 to 1024, as said below
- teacher: float32 [1024, 16, 512], P('tensor', 'dp'), may hold values from -6 to 6
- cotangent: float32 [1024, 16, 512], P('tensor', 'dp'), may hold values from -6 to 6
Outputs:
- output: float32 [1024, 16, 512], P('tensor', 'dp')
- loss: float32 [], replicated
- grad_inputs: float32 [1024, 16, 512], P('tensor', 'dp')
- grad_qkv: float32 [3, 512, 512], P(None, 'dp', 'tensor')
- grad_out_weight: float32 [512, 512], P('tensor', 'dp')
- grad_up: float32 [512, 2048], P('dp', 'tensor')
- grad_down_weight: float32 [2048, 512], P('tensor', 'dp')
- grad_gain_one: float32 [512], replicated
- grad_shift_one: float32 [512], replicated
- grad_gain_two: float32 [512], replicated
- grad_shift_two: float32 [512], replicated
The draws below stay inside these ranges and needn't reach their ends.
Inputs may be any that keep to these rules, and one draw needn't show every extreme that they name: `lengths`: some sequence has exactly 1024 valid tokens and some has exactly 512.
All inputs are finite; a program needn't handle non-finite values.
Results may differ from the reference program's by a relative error of at most 0.006.
The reference program's roundings to bfloat16 on the way count: a program that leaves them out, or rounds other values in their place, can miss the bound.
Values may be sent and summed in bfloat16 or wider, within the bound.
A program may use at most 128 MiB of HBM per device.

```python
import math
import jax
import jax.numpy as jnp
from jax import lax

D = 512
HEADS = 8
HD = 64
FF = 2048
L = 1024
SEQS = 16


def draw_lengths(key, part):
    first_key, second_key = jax.random.split(key)
    lengths_drawn = jax.random.randint(first_key, (SEQS,), L // 2, L + 1)
    chosen = jax.random.permutation(second_key, SEQS)
    lengths_drawn = lengths_drawn.at[chosen[0]].set(L)
    lengths_drawn = lengths_drawn.at[chosen[1]].set(L // 2)
    return lengths_drawn.astype(jnp.int32)


def raised(drawn, stream_key, source, target, parts, factor):
    def block_of(dim):
        return (jnp.arange(drawn.shape[dim]) // (drawn.shape[dim] // parts)).reshape((-1,) + (1,) * (drawn.ndim - 1 - dim))

    first = jax.random.permutation(stream_key, parts)[block_of(target)]
    second = (block_of(target) + parts // 2) % parts
    return jnp.where((block_of(source) == first) | (block_of(source) == second), factor * drawn, drawn)


def levels(own_key, extent, pieces, least, largest):
    def one(position, blocks):
        draws = jax.random.uniform(jax.random.fold_in(jax.random.fold_in(own_key, 6), position), (blocks,), jnp.float32, least / len(pieces), largest / len(pieces))
        return jnp.repeat(jnp.exp(draws), extent[position] // blocks).reshape((-1,) + (1,) * (len(extent) - position - 1))

    level = one(*pieces[0])
    for cut in pieces[1:]:
        level = level * one(*cut)
    return level


def bell_draw(rng, dims, scale, most, cuts=(), held_as=jnp.bfloat16):
    factor_of = levels(rng, dims, cuts, -0.22, 0.18) if cuts else 1.0
    values = jax.random.normal(rng, dims, jnp.float32) * scale * factor_of
    return jnp.minimum(jnp.maximum(values, -most), most).astype(held_as)


def bell_draw_with(key, dims, scale, limit, shards, heavy, kind=jnp.bfloat16):
    values = scale * jax.random.normal(key, dims, jnp.float32)
    if shards:
        values = values * levels(key, dims, shards, -0.22, 0.18)
    return jnp.clip(raised(values, jax.random.fold_in(key, 3), *heavy), -limit, limit).astype(kind)


def setup_inputs(seed: int = 0) -> dict:
    arg_keys = jax.random.split(jax.random.key(seed), 13)
    return {
        "inputs": bell_draw(arg_keys[0], (L, SEQS, D), 1.0, 6.0, ((0, 4), (1, 8)), jnp.float32),
        "qkv_weight": bell_draw(arg_keys[1], (3, D, D), (D // 2) ** -0.5, 0.375, ((1, 8), (2, 4))),
        "out_weight": bell_draw(arg_keys[2], (D, D), (D // 16) ** -0.5, 1.0, ((0, 4), (1, 8))),
        "up_weight": bell_draw(arg_keys[3], (D, FF), D ** -0.5, 0.25, ((0, 8), (1, 4))),
        "down_weight": bell_draw(arg_keys[4], (FF, D), FF ** -0.5, 0.125, ((0, 4), (1, 8))),
        "gain_one": jnp.clip(1.0 + 0.18 * jax.random.normal(arg_keys[5], (D,), jnp.float32), 0.1, 1.9),
        "shift_one": bell_draw(arg_keys[6], (D,), 0.3, 1.5, (), jnp.float32),
        "gain_two": jnp.clip(1.0 + 0.18 * jax.random.normal(arg_keys[7], (D,), jnp.float32), 0.1, 1.9),
        "shift_two": bell_draw(arg_keys[8], (D,), 0.3, 1.5, (), jnp.float32),
        "lengths": draw_lengths(jax.random.fold_in(arg_keys[12], 71), 0),
        "teacher": bell_draw(arg_keys[10], (L, SEQS, D), 1.0, 6.0, ((0, 4), (1, 8)), jnp.float32),
        "cotangent": bell_draw_with(arg_keys[11], (L, SEQS, D), 1.0, 6.0, ((0, 4), (1, 8)), (1, 2, 8, 2.0), jnp.float32),
    }


@jax.custom_vjp
def low(v):
    return lax.optimization_barrier(v.astype(jnp.bfloat16)).astype(jnp.float32)

@jax.custom_vjp
def lowered_backward(v):
    return v

def low_keep(v):
    return (low(v), None)

def low_pass(kept, grad):
    return (grad,)

def back_keep(v):
    return (v, None)

def back_low(kept, grad):
    return (low(grad),)
low.defvjp(low_keep, low_pass)
lowered_backward.defvjp(back_keep, back_low)

def norm_rows(values, gain, shift):
    center = values - lax.optimization_barrier(jnp.mean(values, -1, keepdims=True))
    spread = lax.optimization_barrier(jnp.mean(center * center, -1, keepdims=True))
    return center * lax.rsqrt(spread + 1e-05) * gain + shift

def angle_tables(positions, width):
    half = width // 2
    rates = jnp.exp(jnp.arange(half, dtype=jnp.float32) * (-2.0 * math.log(10000.0) / width))
    angles = positions.astype(jnp.float32)[:, None] * rates[None, :]
    cosine = jnp.concatenate([jnp.cos(angles), jnp.cos(angles)], -1)[:, None, None, :]
    sine = jnp.concatenate([jnp.sin(angles), jnp.sin(angles)], -1)[:, None, None, :]
    return (cosine, sine)

def turn_half(values):
    half = values.shape[-1] // 2
    return jnp.concatenate([-values[..., half:], values[..., :half]], -1)

def rotate(values, cosine, sine):
    return values * cosine + turn_half(values) * sine

def reference(inputs, qkv_weight, out_weight, up_weight, down_weight, gain_one, shift_one, gain_two, shift_two, lengths, teacher, cotangent):
    positions = jnp.arange(L)
    valid = (positions[:, None] < lengths[None, :]).astype(jnp.float32)[:, :, None]
    total = jnp.sum(lengths).astype(jnp.float32)
    factor = L * SEQS / total
    cosine, sine = angle_tables(positions, HD)
    scale = HD ** (-0.5)
    exact_gelu_flag = lax.Precision.HIGHEST

    def attend(packed):
        queries, keys_all, values_all, length = packed
        raw = lowered_backward(jnp.einsum('qhe,khe->hqk', queries, keys_all, precision=exact_gelu_flag))
        allowed = (positions[None, :] <= positions[:, None]) & (positions[None, :] < length)
        scores = jnp.where(allowed[None], raw * scale, -1e+30)
        highest = lax.optimization_barrier(jnp.max(scores, -1, keepdims=True))
        expd = jnp.exp(scores - highest)
        probs = expd / lax.optimization_barrier(jnp.sum(expd, -1, keepdims=True))
        return jnp.einsum('hqk,khe->qhe', low(probs), values_all, precision=exact_gelu_flag)

    def forward(x_in, w_qkv, w_out, up_matrix, down_matrix, g_one, b_one, g_two, b_two):
        normed = low(norm_rows(x_in, g_one, b_one))
        projected = jnp.einsum('lsd,cdk->clsk', normed, w_qkv, precision=exact_gelu_flag).reshape(3, L, SEQS, HEADS, HD)
        queries = low(rotate(lowered_backward(projected[0]), cosine, sine))
        keys_all = low(rotate(lowered_backward(projected[1]), cosine, sine))
        values_all = low(lowered_backward(projected[2]))
        mixed = lax.map(jax.checkpoint(attend), (jnp.transpose(queries, (1, 0, 2, 3)), jnp.transpose(keys_all, (1, 0, 2, 3)), jnp.transpose(values_all, (1, 0, 2, 3)), lengths))
        attended = low(lowered_backward(jnp.transpose(mixed, (1, 0, 2, 3)).reshape(L, SEQS, D)))
        middle_state = x_in + lowered_backward(jnp.einsum('lsk,kd->lsd', attended, w_out, precision=exact_gelu_flag))
        second_normed_rows = low(norm_rows(middle_state, g_two, b_two))
        activation_input = lowered_backward(jnp.einsum('agm,mt->agt', second_normed_rows, up_matrix, precision=exact_gelu_flag))
        hidden_rows = low(jax.nn.gelu(activation_input, approximate=False))
        output = middle_state + lowered_backward(jnp.einsum('bzv,vc->bzc', hidden_rows, down_matrix, precision=exact_gelu_flag))
        differ = output - teacher
        objective = factor * jnp.sum(valid * (cotangent * output + 0.5 * differ * differ))
        loss = jnp.sum(valid * differ * differ) / (total * D)
        return (objective, (output, loss))
    floats = (inputs, qkv_weight.astype(jnp.float32), out_weight.astype(jnp.float32), up_weight.astype(jnp.float32), down_weight.astype(jnp.float32), gain_one, shift_one, gain_two, shift_two)
    objective, pullback, extras = jax.vjp(forward, *floats, has_aux=True)
    grads = pullback(jnp.ones_like(objective))
    return (extras[0], extras[1], grads[0], grads[1], grads[2], grads[3], grads[4], grads[5], grads[6], grads[7], grads[8])
```

```python
import math

import jax
import jax.numpy as jnp
import numpy as np
from jax import lax
from jax.experimental import pallas as pl
from jax.experimental.pallas import tpu as pltpu
from jax.sharding import PartitionSpec as P

HD = 64
F32 = jnp.float32
BF16 = jnp.bfloat16
MESH = pl.DeviceIdType.MESH
VMEM_LIMIT = 60 * 1024 * 1024

NN = (((1,), (0,)), ((), ()))
NT = (((1,), (1,)), ((), ()))


def dot(a, b, dims=NN):
    return lax.dot_general(a, b, dims, preferred_element_type=F32)


class Place:
    def __init__(self, sizes):
        dp, tensor = lax.axis_index("dp"), lax.axis_index("tensor")
        self.sizes = sizes
        self.at = {"z": dp // sizes["y"], "y": dp % sizes["y"], "x": tensor // 2, "c": tensor % 2}

    def moved(self, axis, delta):
        size = self.sizes[axis]
        if size == 2:
            return 1 - self.at[axis]
        return lax.rem(self.at[axis] + (delta % size), size)

    def device(self, **moves):
        at = dict(self.at)
        for axis, delta in moves.items():
            at[axis] = self.moved(axis, delta)
        return (at["z"] * self.sizes["y"] + at["y"], at["x"] * 2 + at["c"])

    def peers(self):
        out = [self.device(x=1), self.device(c=1), self.device(x=1, c=1), self.device(y=1)]
        out += [self.device(z=delta) for delta in range(1, self.sizes["z"])]
        return out

    def meet(self):
        barrier = pltpu.get_barrier_semaphore()
        peers = self.peers()
        for peer in peers:
            pl.semaphore_signal(barrier, inc=1, device_id=peer, device_id_type=MESH)
        return lambda: pl.semaphore_wait(barrier, len(peers))


def remote(src, dst, send, recv, device):
    return pltpu.make_async_remote_copy(
        src_ref=src, dst_ref=dst, send_sem=send, recv_sem=recv, device_id=device, device_id_type=MESH
    )


class Gather:
    def __init__(self, place, view, order, send, recv, base):
        self.place, self.view, self.order = place, view, order
        self.send, self.recv, self.base = send, recv, base
        self.have = {}
        self.open = []
        self.sent = []

    @staticmethod
    def count(sizes, order):
        return sum(sizes[axis] - 1 for axis in order)

    def part(self, **changed):
        where = dict(self.place.at)
        where.update(self.have)
        where.update(changed)
        return self.view(where)

    def start(self):
        axis = self.order[0]
        size = self.place.sizes[axis]
        mine = self.part()
        self.open = []
        for delta in range(1, size):
            slot = self.base
            self.base += 1
            copy = remote(mine, mine, self.send.at[slot], self.recv.at[slot], self.place.device(**{axis: delta}))
            copy.start()
            theirs = self.part(**{axis: self.place.moved(axis, -delta)})
            self.open.append(
                remote(theirs, theirs, self.send.at[slot], self.recv.at[slot], self.place.device(**{axis: delta}))
            )
            self.sent.append(copy)

    def arrive(self):
        for copy in self.open:
            copy.wait_recv()
        self.open = []
        self.have[self.order[0]] = slice(None)
        self.order = self.order[1:]

    def finish(self):
        for copy in self.sent:
            copy.wait_send()
        self.sent = []


def lanes(shape, limit):
    return lax.broadcasted_iota(jnp.int32, shape, 1) < limit


def token_rows(ref, seq, rows):
    return [ref[pl.ds(2 * j + seq, rows, stride=8), :] for j in range(4)]


def row_mean(parts):
    total = parts[0]
    for part in parts[1:]:
        total = total + part
    return jnp.sum(total, -1, keepdims=True) * (1.0 / (128 * len(parts)))


def normalize(parts):
    mean = row_mean(parts)
    center = [part - mean for part in parts]
    spread = row_mean([part * part for part in center])
    scale = lax.rsqrt(spread + 1e-05)
    return center, scale


def rope(value, cos, sin_a, sin_b):
    return value * cos + pltpu.roll(value, 96, 1) * sin_a + pltpu.roll(value, 32, 1) * sin_b


def rope_back(grad, cos, sin_a, sin_b):
    return grad * cos - pltpu.roll(grad, 96, 1) * sin_a - pltpu.roll(grad, 32, 1) * sin_b


def rope_tables(rows):
    half = HD // 2
    rates = np.exp(np.arange(half, dtype=np.float32) * np.float32(-2.0 * math.log(10000.0) / HD))
    angles = np.arange(rows, dtype=np.float32)[:, None] * rates.astype(np.float32)[None, :]
    cos, sin, zero = np.cos(angles), np.sin(angles), np.zeros_like(angles)
    tables = [[cos] * 4, [-sin, zero] * 2, [zero, sin] * 2]
    return jnp.asarray(np.stack([np.concatenate(table, -1) for table in tables]).astype(np.float32))


def front_kernel(
    sizes,
    rows,
    block,
    lengths,
    x_ref,
    qkv_shard,
    out_shard,
    up_shard,
    down_shard,
    gain,
    shift,
    tables,
    ff_all,
    out_all,
    qkv_all,
    counts,
    normed_all,
    q_all,
    k_all,
    v_all,
    lse,
    attended,
    own_normed,
    own_attended,
    local_sem,
    send,
    recv,
    send2,
    recv2,
):
    place = Place(sizes)
    at = place.at
    x, c, z, y = at["x"], at["c"], at["z"], at["y"]
    own = rows // 4
    met = place.meet()

    def ff_view(w):
        return ff_all.at[w["x"], w["c"], w["z"], w["y"]]

    def local(index, src, dst):
        copy = pltpu.make_async_copy(src, dst, local_sem.at[index])
        copy.start()
        return copy

    def x_lane(index):
        return pl.ds(pl.multiple_of(index * 128, 128), 128)

    def out_at(w):
        lane = slice(None) if isinstance(w["x"], slice) else x_lane(w["x"])
        return out_all.at[w["c"], w["z"], w["y"], :, lane]

    def qkv_at(w):
        lane = slice(None) if isinstance(w["x"], slice) else x_lane(w["x"])
        return qkv_all.at[:, w["z"], w["y"], :, lane]

    copies = [
        local(0, qkv_shard, qkv_at(at)),
        local(1, out_shard, out_at(at)),
        local(2, up_shard, ff_all.at[x, c, z, y, :, pl.ds(0, 512)]),
        local(3, down_shard, ff_all.at[x, c, z, y, :, pl.ds(512, 512)]),
    ]
    total = lengths[0]
    for s in range(1, 2):
        total = total + lengths[s]
    counts[z, y] = jnp.full((8, 128), total.astype(F32))

    base = 0
    plans = []
    for view, order in (
        (qkv_at, "zyx"),
        (out_at, "zyxc"),
        (ff_view, "zyxc"),
        (lambda w: counts.at[w["z"], w["y"]], "zy"),
    ):
        plans.append(Gather(place, view, order, send, recv, base))
        base += Gather.count(sizes, order)
    qkv_g, out_g, ff_g, count_g = plans

    for s in range(2):
        center, scale = normalize(token_rows(x_ref, s, own))
        for j in range(4):
            lane = pl.ds(128 * j, 128)
            value = center[j] * scale * gain[:, lane] + shift[:, lane]
            own_normed[s, :, lane] = value.astype(BF16)
    for copy in copies:
        copy.wait()
    met()
    mine = pl.ds(pl.multiple_of((x * 2 + c) * own, own), own)
    keep = local(0, own_normed.at[x], normed_all.at[mine])
    tokens = []
    for index, (seq, moves) in enumerate(((1 - x, {"x": 1}), (1 - x, {"x": 1, "c": 1}), (x, {"c": 1}))):
        copy = remote(own_normed.at[seq], normed_all.at[mine], send2.at[index], recv2.at[index], place.device(**moves))
        copy.start()
        who = dict(at)
        for axis in moves:
            who[axis] = 1 - at[axis]
        theirs = normed_all.at[pl.ds(pl.multiple_of((who["x"] * 2 + who["c"]) * own, own), own)]
        tokens.append((copy, remote(theirs, theirs, send2.at[index], recv2.at[index], place.device(**moves))))
    qkv_g.start()
    count_g.start()
    qkv_g.arrive()
    qkv_g.start()
    count_g.arrive()
    count_g.start()
    qkv_g.arrive()
    qkv_g.start()
    out_g.start()
    ff_g.start()
    keep.wait()
    for sent, came in tokens:
        came.wait_recv()
    qkv_g.arrive()

    w_qkv = [qkv_all[i].reshape(-1, 256) for i in range(3)]

    def project(index, carry):
        here = pl.ds(pl.multiple_of(index * block, block), block)
        normed = normed_all[here, :]
        cos, sin_a, sin_b = (tables[i, here, :] for i in range(3))
        for i, ref in ((0, q_all), (1, k_all), (2, v_all)):
            value = dot(normed, w_qkv[i])
            for pair in range(2):
                lane = pl.ds(128 * pair, 128)
                part = value[:, 128 * pair : 128 * pair + 128]
                if i < 2:
                    part = rope(part, cos, sin_a, sin_b)
                if i == 0:
                    part = part.astype(BF16) * jnp.asarray(HD**-0.5, BF16)
                ref[here, lane] = part.astype(BF16)
        return carry

    lax.fori_loop(0, rows // block, project, 0)
    count_g.arrive()
    out_g.arrive()
    out_g.start()
    ff_g.arrive()
    ff_g.start()

    length = lengths[x]
    half = lanes((block, 128), HD)
    zero = jnp.zeros((block, 128), BF16)

    def attend(pair, carry):
        lane = pl.ds(pl.multiple_of(pair * 128, 128), 128)
        for qb in range(rows // block):
            here = pl.ds(qb * block, block)
            keys = (qb + 1) * block
            queries = q_all[here, lane]
            k_part = k_all[pl.ds(0, keys), lane]
            v_part = v_all[pl.ds(0, keys), lane]
            key_pos = lax.broadcasted_iota(jnp.int32, (block, keys), 1)
            query_pos = lax.broadcasted_iota(jnp.int32, (block, keys), 0) + qb * block
            allowed = key_pos <= query_pos
            if keys > rows // 2:
                allowed = allowed & (key_pos < length)
            mixed = []
            for head in range(2):
                masked = jnp.where(half, queries, zero) if head == 0 else jnp.where(half, zero, queries)
                scores = jnp.where(allowed, dot(masked, k_part, NT), -1e30)
                highest = jnp.max(scores, -1, keepdims=True)
                expd = jnp.exp(scores - highest)
                denom = jnp.sum(expd, -1, keepdims=True)
                probs = (expd * (1.0 / denom)).astype(BF16)
                mixed.append(dot(probs, v_part))
                wide = jnp.broadcast_to(highest + jnp.log(denom), (block, 128))
                lse[pair * 2 + head, :, here] = jnp.transpose(wide)[:8]
            own_attended[here, lane] = jnp.where(half, mixed[0], mixed[1]).astype(BF16)
        return carry

    lax.fori_loop(0, 2, attend, 0)
    out_g.arrive()
    out_g.start()
    ff_g.arrive()
    ff_g.start()

    def rows_of(tx, tc):
        return pl.ds(pl.multiple_of((tx * 2 + tc) * own, own), own)

    keep2 = local(1, own_attended.at[rows_of(x, c)], attended.at[c, x])
    moved = []
    for index, moves in enumerate(({"x": 1}, {"x": 1, "c": 1}, {"c": 1})):
        to = dict(at)
        for axis in moves:
            to[axis] = 1 - at[axis]
        copy = remote(
            own_attended.at[rows_of(to["x"], to["c"])],
            attended.at[c, x],
            send2.at[3 + index],
            recv2.at[3 + index],
            place.device(**moves),
        )
        copy.start()
        theirs = attended.at[to["c"], to["x"]]
        moved.append((copy, remote(theirs, theirs, send2.at[3 + index], recv2.at[3 + index], place.device(**moves))))
    out_g.arrive()
    out_g.start()
    ff_g.arrive()
    ff_g.start()
    keep2.wait()
    for sent, came in moved:
        came.wait_recv()
    out_g.arrive()
    ff_g.arrive()
    for plan in plans:
        plan.finish()
    for sent, came in tokens + moved:
        sent.wait_send()


def front(sizes, rows, lengths, x, qkv, out, up, down, gain, shift, tables):
    zs, ys = sizes["z"], sizes["y"]
    shard = qkv.shape[1]
    own = rows // 4
    block = 256
    orders = ("zyx", "zyxc", "zyxc", "zy")
    slots = sum(Gather.count(sizes, order) for order in orders)
    any_spec = pl.BlockSpec(memory_space=pl.ANY)
    vmem = pl.BlockSpec(memory_space=pltpu.VMEM)
    shapes = [
        ((2, 2, zs, ys, shard, 1024), BF16),
        ((2, zs, ys, shard, 256), BF16),
        ((3, zs, ys, shard, 256), BF16),
        ((zs, ys, 8, 128), F32),
        ((rows, 512), BF16),
        ((rows, 256), BF16),
        ((rows, 256), BF16),
        ((rows, 256), BF16),
        ((4, 8, rows), F32),
        ((2, 2, own, 256), BF16),
    ]
    return pl.pallas_call(
        lambda *refs: front_kernel(sizes, rows, block, *refs),
        out_shape=[jax.ShapeDtypeStruct(*shape) for shape in shapes],
        in_specs=[pl.BlockSpec(memory_space=pltpu.SMEM), vmem] + [any_spec] * 4 + [vmem] * 3,
        out_specs=[vmem] * len(shapes),
        scratch_shapes=[
            pltpu.VMEM((2, own, 512), BF16),
            pltpu.VMEM((rows, 256), BF16),
            pltpu.SemaphoreType.DMA((4,)),
            pltpu.SemaphoreType.DMA((slots,)),
            pltpu.SemaphoreType.DMA((slots,)),
            pltpu.SemaphoreType.DMA((6,)),
            pltpu.SemaphoreType.DMA((6,)),
        ],
        name="front",
        compiler_params=pltpu.CompilerParams(
            collective_id=0, has_side_effects=True, vmem_limit_bytes=VMEM_LIMIT
        ),
    )(lengths, x, qkv, out, up, down, gain, shift, tables)


def gelu_parts(value):
    cdf = 0.5 + 0.5 * lax.erf(value * (2.0**-0.5))
    density = jnp.exp(-0.5 * value * value) * ((2.0 * math.pi) ** -0.5)
    return value * cdf, cdf + value * density


def middle_kernel(
    own,
    tensor_total,
    lengths,
    counts,
    x_ref,
    teacher,
    cotangent,
    attended,
    ff_all,
    out_all,
    gain,
    shift,
    output,
    grad_middle,
    grad_attended,
    grad_ff,
    grad_out,
    stats,
    middle,
    seed,
    slope,
    hidden,
    total_sum,
):
    tokens = 2 * own
    tensor = lax.axis_index("tensor")
    count = jnp.sum(counts[...], axis=0)[0:1]
    factor = tensor_total / count
    valid = []
    for s in range(2):
        rows = pl.ds(s * own, own)
        attn = dot(attended[0, s], out_all[0], NT) + dot(attended[1, s], out_all[1], NT)
        parts = token_rows(x_ref, s, own)
        for j in range(4):
            middle[rows, pl.ds(128 * j, 128)] = parts[j] + attn[:, 128 * j : 128 * j + 128]
        position = tensor * own + lax.broadcasted_iota(jnp.int32, (own, 128), 0)
        valid.append((position < lengths[s]).astype(F32))
    value = middle[...]
    mean = jnp.mean(value, -1, keepdims=True)
    center = value - mean
    scale = lax.rsqrt(jnp.mean(center * center, -1, keepdims=True) + 1e-05)
    normed = (center * scale * gain[...] + shift[...]).astype(BF16)
    normed_t = jnp.transpose(normed)

    total_sum[...] = jnp.zeros_like(total_sum)

    def up(t, carry):
        before = dot(normed, ff_all[t, :, pl.ds(0, 512)])
        act, slope_t = gelu_parts(before)
        act = act.astype(BF16)
        slope[t] = slope_t
        hidden[t] = act
        total_sum[...] += dot(act, ff_all[t, :, pl.ds(512, 512)], NT)
        return carry

    lax.fori_loop(0, 4, up, 0)

    square = jnp.zeros((own, 128), F32)
    for s in range(2):
        rows = pl.ds(s * own, own)
        want = token_rows(teacher, s, own)
        weight = token_rows(cotangent, s, own)
        for j in range(4):
            lane = pl.ds(128 * j, 128)
            out = middle[rows, lane] + total_sum[rows, lane]
            output[pl.ds(2 * j + s, own, stride=8), :] = out
            differ = out - want[j]
            square = square + valid[s] * differ * differ
            seed[rows, lane] = factor * valid[s] * (weight[j] + differ)
    grad_f = seed[...].astype(BF16)
    grad_f_t = jnp.transpose(grad_f)
    total_sum[...] = jnp.zeros_like(total_sum)

    def down(t, carry):
        grad_hidden = dot(grad_f, ff_all[t, :, pl.ds(512, 512)])
        grad_before = (slope[t] * grad_hidden).astype(BF16)
        grad_ff[t, :, pl.ds(0, 512)] = dot(normed_t, grad_before).astype(BF16)
        grad_ff[t, :, pl.ds(512, 512)] = dot(grad_f_t, hidden[t]).astype(BF16)
        total_sum[...] += dot(grad_before, ff_all[t, :, pl.ds(0, 512)], NT)
        return carry

    lax.fori_loop(0, 4, down, 0)

    grad_normed = total_sum[...]
    unit = (middle[...] - mean) * scale
    stats[...] = jnp.zeros_like(stats)
    stats[0:1, 0:128] = jnp.sum(square, 0, keepdims=True)
    stats[8:9] = jnp.sum(grad_normed * unit, 0, keepdims=True)
    stats[16:17] = jnp.sum(grad_normed, 0, keepdims=True)
    scaled = grad_normed * gain[...]
    inner = jnp.mean(scaled * unit, -1, keepdims=True)
    grad = seed[...] + scale * (scaled - jnp.mean(scaled, -1, keepdims=True) - unit * inner)
    grad_middle[...] = grad
    branch = grad.astype(BF16)
    branch_t = jnp.transpose(branch)
    for k in range(2):
        grad_out[k] = (dot(branch_t[:, :own], attended[k, 0]) + dot(branch_t[:, own:], attended[k, 1])).astype(BF16)
        back = dot(branch, out_all[k]).astype(BF16)
        for s in range(2):
            grad_attended[k, s] = back[s * own : s * own + own]


def middle_part(own, tensor_total, lengths, counts, x, teacher, cotangent, attended, ff_all, out_all, gain, shift):
    tokens = 2 * own
    vmem = pl.BlockSpec(memory_space=pltpu.VMEM)
    shapes = [
        (x.shape, F32),
        ((tokens, 512), F32),
        ((2, 2, own, 256), BF16),
        ((4, 512, 1024), BF16),
        ((2, 512, 256), BF16),
        ((24, 512), F32),
    ]
    return pl.pallas_call(
        lambda *refs: middle_kernel(own, tensor_total, *refs),
        out_shape=[jax.ShapeDtypeStruct(*shape) for shape in shapes],
        in_specs=[pl.BlockSpec(memory_space=pltpu.SMEM)] + [vmem] * 9,
        out_specs=[vmem] * len(shapes),
        scratch_shapes=[
            pltpu.VMEM((tokens, 512), F32),
            pltpu.VMEM((tokens, 512), F32),
            pltpu.VMEM((4, tokens, 512), F32),
            pltpu.VMEM((4, tokens, 512), BF16),
            pltpu.VMEM((tokens, 512), F32),
        ],
        name="middle",
        compiler_params=pltpu.CompilerParams(vmem_limit_bytes=VMEM_LIMIT),
    )(lengths, counts, x, teacher, cotangent, attended, ff_all, out_all, gain, shift)


class Scatter:
    def __init__(self, place, view, order, landing, send, recv, base):
        self.place, self.view, self.order, self.landing = place, view, order, landing
        self.send, self.recv, self.base = send, recv, base
        self.left = list(order)
        self.where = dict(place.at)
        for axis in order:
            self.where[axis] = slice(None)
        self.open = []
        self.sent = []

    def part(self, view=None, **changed):
        where = dict(self.where)
        where.update(changed)
        return (view or self.view)(where)

    def start(self):
        axis = self.left[0]
        phase = len(self.order) - len(self.left)
        self.open = []
        for delta in range(1, self.place.sizes[axis]):
            slot = self.base
            self.base += 1
            source = self.part(**{axis: self.place.moved(axis, delta)})
            copy = remote(
                source,
                self.landing[phase].at[delta - 1],
                self.send.at[slot],
                self.recv.at[slot],
                self.place.device(**{axis: delta}),
            )
            copy.start()
            self.open.append(copy)
            self.sent.append(copy)

    def arrive(self, final=None):
        axis = self.left[0]
        phase = len(self.order) - len(self.left)
        for copy in self.open:
            copy.wait_recv()
        count = len(self.open)
        self.open = []
        self.where[axis] = self.place.at[axis]
        self.left = self.left[1:]
        rest = [a for a in "xczy" if a in self.left and not (a == "x" and self.lane_x)]
        sizes = [self.place.sizes[a] for a in rest]
        landing = self.landing[phase]

        def add(index, carry):
            chosen = {}
            for a, size in zip(reversed(rest), reversed(sizes)):
                chosen[a] = lax.rem(index, size)
                index = index // size
            mine = self.part(**chosen)
            total = mine[...].astype(F32)
            kept = self.part(view=self.work, **chosen) if self.work else mine
            for i in range(count):
                piece = landing.at[i]
                total = total + self.piece(piece, chosen, rest)[...].astype(F32)
            if final is None:
                kept[...] = total.astype(BF16)
            else:
                final[...] = total
            return carry

        steps = math.prod(sizes)
        if steps == 1:
            add(0, 0)
        else:
            lax.fori_loop(0, steps, add, 0)
        if self.work:
            self.view, self.work = self.work, None

    lane_x = False
    lead = 0
    work = None

    def piece(self, landing, chosen, rest):
        index = (slice(None),) * self.lead + tuple(chosen[a] for a in rest)
        return landing.at[index] if index else landing

    def finish(self):
        for copy in self.sent:
            copy.wait_send()


def landing_shapes(sizes, order, dims, tail, lead=(), lane_x=0):
    left = list(order)
    shapes = []
    for axis in order:
        left.remove(axis)
        shape = (sizes[axis] - 1,) + lead + tuple(sizes[a] for a in dims if a in left)
        wide = tail[1]
        if lane_x:
            wide = lane_x * (2 if "x" in left else 1)
        shapes.append(shape + (tail[0], wide))
    return shapes


UP_ORDER, DOWN_ORDER, OUT_ORDER, QKV_ORDER = "cxyz", "cyxz", "cxyz", "xyz"


def back_kernel(
    sizes,
    rows,
    block,
    lengths,
    grad_attended,
    q_all,
    k_all,
    v_all,
    lse,
    normed_all,
    qkv_all,
    grad_middle,
    x_ref,
    gain,
    tables,
    grad_ff,
    grad_out,
    stats,
    grad_inputs,
    up_final,
    down_final,
    out_final,
    qkv_final,
    stats_final,
    g_all,
    k_t,
    grad_q,
    grad_k,
    grad_v,
    grad_proj,
    grad_qkv,
    grad_n,
    ff_work,
    out_work,
    from_core,
    to_x,
    from_x,
    stat_send,
    stat_land,
    local_sem,
    send,
    recv,
    send2,
    recv2,
    *landing,
):
    place = Place(sizes)
    at = place.at
    x, c, z, y = at["x"], at["c"], at["z"], at["y"]
    own = rows // 4
    met = place.meet()

    def mine(tx, tc):
        return pl.ds(pl.multiple_of((tx * 2 + tc) * own, own), own)

    def x_lane(index):
        if isinstance(index, slice):
            return index
        return pl.ds(pl.multiple_of(index * 128, 128), 128)

    def half_view(start):
        return lambda w: grad_ff.at[w["x"], w["c"], w["z"], w["y"], :, pl.ds(start, 512)]

    def out_view(w):
        return grad_out.at[w["c"], w["z"], w["y"], :, x_lane(w["x"])]

    def qkv_view(w):
        return grad_qkv.at[:, w["z"], w["y"], :, x_lane(w["x"])]

    base = 0
    plans = []
    used = 0
    for view, order, lead, lane_x in (
        (half_view(0), UP_ORDER, 0, False),
        (half_view(512), DOWN_ORDER, 0, False),
        (out_view, OUT_ORDER, 0, True),
        (qkv_view, QKV_ORDER, 1, True),
    ):
        plan = Scatter(place, view, order, landing[used : used + len(order)], send, recv, base)
        plan.lead, plan.lane_x = lead, lane_x
        plans.append(plan)
        used += len(order)
        base += sum(sizes[axis] - 1 for axis in order)
    up_s, down_s, out_s, qkv_s = plans
    up_s.work = lambda w: ff_work.at[w["x"], w["z"], w["y"], :, pl.ds(0, 512)]
    down_s.work = lambda w: ff_work.at[w["x"], w["z"], w["y"], :, pl.ds(512, 512)]
    out_s.work = lambda w: out_work.at[w["z"], w["y"], :, x_lane(w["x"])]

    met()
    keep = pltpu.make_async_copy(grad_attended.at[c, x], g_all.at[mine(x, c)], local_sem.at[0])
    keep.start()
    moved = []
    for index, moves in enumerate(({"x": 1}, {"x": 1, "c": 1}, {"c": 1})):
        to = dict(at)
        for axis in moves:
            to[axis] = 1 - at[axis]
        copy = remote(
            grad_attended.at[to["c"], to["x"]],
            g_all.at[mine(x, c)],
            send2.at[index],
            recv2.at[index],
            place.device(**moves),
        )
        copy.start()
        theirs = g_all.at[mine(to["x"], to["c"])]
        moved.append((copy, remote(theirs, theirs, send2.at[index], recv2.at[index], place.device(**moves))))
    for plan in (up_s, down_s, out_s):
        plan.start()
    for pair in range(2):
        k_t[pair] = jnp.transpose(k_all[:, pl.ds(128 * pair, 128)])
    normed_t = jnp.transpose(normed_all[...])
    keep.wait()
    for sent, came in moved:
        came.wait_recv()

    length = lengths[x]
    half = lanes((block, 128), HD)
    zero = jnp.zeros((block, 128), BF16)
    upper = lax.broadcasted_iota(jnp.int32, (128, block), 0) < HD

    def attend(pair, blocks):
        lane = pl.ds(128 * pair, 128)
        for qb in blocks:
            here = pl.ds(qb * block, block)
            keys = (qb + 1) * block
            seen = pl.ds(0, keys)
            queries = q_all[here, lane]
            grads = g_all[here, lane]
            k_part = k_all[seen, lane]
            v_part = v_all[seen, lane]
            key_pos = lax.broadcasted_iota(jnp.int32, (keys, block), 0)
            query_pos = lax.broadcasted_iota(jnp.int32, (keys, block), 1) + qb * block
            allowed = key_pos <= query_pos
            if keys > rows // 2:
                allowed = allowed & (key_pos < length)
            dq = []
            for head in range(2):
                if head == 0:
                    q_m, g_m = jnp.where(half, queries, zero), jnp.where(half, grads, zero)
                else:
                    q_m, g_m = jnp.where(half, zero, queries), jnp.where(half, zero, grads)
                scores = dot(k_part, q_m, NT)
                probs = jnp.where(allowed, jnp.exp(scores - lse[pair * 2 + head, 0:1, here]), 0.0)
                grad_probs = dot(v_part, g_m, NT)
                inner = jnp.sum(probs * grad_probs, 0, keepdims=True)
                grad_raw = (probs * (grad_probs - inner)).astype(BF16)
                add_k = dot(grad_raw, q_m)
                add_v = dot(probs.astype(BF16), g_m)
                if qb == rows // block - 1 and head == 0:
                    grad_k[seen, lane] = add_k
                    grad_v[seen, lane] = add_v
                else:
                    grad_k[seen, lane] += add_k
                    grad_v[seen, lane] += add_v
                dq.append(dot(k_t[pair, :, seen], grad_raw))
            grad_q[here, lane] = jnp.transpose(jnp.where(upper, dq[0], dq[1])) * HD**-0.5

    last = rows // block - 1
    attend(0, [last])
    for plan in (up_s, down_s, out_s):
        plan.arrive()
        plan.start()
    attend(0, range(last - 1, -1, -1))
    attend(1, [last])
    for plan in (out_s, up_s, down_s):
        plan.arrive()
        plan.start()
    attend(1, range(last - 1, -1, -1))

    def turned(index, carry):
        here = pl.ds(pl.multiple_of(index * block, block), block)
        cos, sin_a, sin_b = (tables[i, here, :] for i in range(3))
        total = jnp.zeros((block, 512), F32)
        for i, ref in ((0, grad_q), (1, grad_k), (2, grad_v)):
            for pair in range(2):
                lane = pl.ds(128 * pair, 128)
                part = ref[here, lane]
                if i < 2:
                    part = rope_back(part, cos, sin_a, sin_b)
                grad_proj[i, here, lane] = part.astype(BF16)
            total = total + dot(grad_proj[i, here, :], qkv_all[i], NT)
        grad_n[here, :] = total
        return carry

    lax.fori_loop(0, rows // block, turned, 0)
    core = []
    for i in range(2):
        copy = remote(
            grad_n.at[mine(i, 1 - c)], from_core.at[i], send2.at[3 + i], recv2.at[3 + i], place.device(c=1)
        )
        copy.start()
        core.append(copy)
    deep = sizes["z"] * sizes["y"]
    shard = 512 // deep
    for i in range(3):
        value = dot(normed_t, grad_proj[i]).astype(BF16)
        grad_qkv[i] = value.reshape(sizes["z"], sizes["y"], shard, 256)
    for copy in core:
        copy.wait_recv()
    to_x[...] = (grad_n[mine(1 - x, c), :] + from_core[1 - x]).astype(BF16)
    cross = remote(to_x, from_x, send2.at[5], recv2.at[5], place.device(x=1))
    cross.start()
    qkv_s.start()
    for plan in (out_s, up_s, down_s):
        plan.arrive()
        plan.start()
    stat_send[0] = jnp.zeros_like(stat_send[0])
    stat_send[0, 0:24] = stats[...]
    cross.wait_recv()
    grad_gain = [jnp.zeros((1, 128), F32)] * 4
    grad_shift = [jnp.zeros((1, 128), F32)] * 4
    for s in range(2):
        center, scale = normalize(token_rows(x_ref, s, own))
        local = grad_n[mine(x, c), :] + from_core[x]
        far = from_x[...].astype(F32)
        chosen = jnp.where(x == s, local, far)
        grads = [chosen[:, 128 * j : 128 * j + 128] for j in range(4)]
        units = [part * scale for part in center]
        scaled = [grads[j] * gain[:, pl.ds(128 * j, 128)] for j in range(4)]
        mean = row_mean(scaled)
        inner = row_mean([scaled[j] * units[j] for j in range(4)])
        for j in range(4):
            part = grad_middle[pl.ds(s * own, own), pl.ds(128 * j, 128)]
            grad_inputs[pl.ds(2 * j + s, own, stride=8), :] = part + scale * (scaled[j] - mean - units[j] * inner)
            grad_gain[j] = grad_gain[j] + jnp.sum(grads[j] * units[j], 0, keepdims=True)
            grad_shift[j] = grad_shift[j] + jnp.sum(grads[j], 0, keepdims=True)
    for j in range(4):
        stat_send[0, 24:25, 128 * j : 128 * j + 128] = grad_gain[j]
        stat_send[0, 32:33, 128 * j : 128 * j + 128] = grad_shift[j]

    slot = 6
    landed = 0
    stat_sent = []
    for phase, axis in enumerate("cxyz"):
        came = []
        for delta in range(1, sizes[axis]):
            copy = remote(
                stat_send.at[phase], stat_land.at[landed], send2.at[slot], recv2.at[slot], place.device(**{axis: delta})
            )
            copy.start()
            came.append((copy, landed))
            stat_sent.append(copy)
            slot += 1
            landed += 1
        if phase < 3:
            qkv_s.arrive(None if phase < 2 else qkv_final)
            if phase < 2:
                qkv_s.start()
        if phase == 1:
            out_s.arrive(out_final)
            up_s.arrive(up_final)
            down_s.arrive(down_final)
        total = stat_send[phase]
        for copy, index in came:
            copy.wait_recv()
            total = total + stat_land[index]
        if phase < 3:
            stat_send[phase + 1] = total
        else:
            stats_final[...] = total
    for plan in plans:
        plan.finish()
    for copy in [sent for sent, _ in moved] + core + [cross] + stat_sent:
        copy.wait_send()


def back(sizes, rows, lengths, grad_attended, q, k, v, lse, normed, qkv, grad_middle, x, gain, tables, grad_ff, grad_out, stats):
    zs, ys = sizes["z"], sizes["y"]
    shard = 512 // (zs * ys)
    own = rows // 4
    block = 256
    vmem = pl.BlockSpec(memory_space=pltpu.VMEM)
    shapes = [x.shape, (shard, 512), (shard, 512), (shard, 128), (3, shard, 128), (40, 512)]
    lands = landing_shapes(sizes, UP_ORDER, "xczy", (shard, 512))
    lands += landing_shapes(sizes, DOWN_ORDER, "xczy", (shard, 512))
    lands += landing_shapes(sizes, OUT_ORDER, "czy", (shard, 256), lane_x=128)
    lands += landing_shapes(sizes, QKV_ORDER, "zy", (shard, 256), lead=(3,), lane_x=128)
    slots = sum(shape[0] for shape in lands)
    meets = sum(sizes[axis] - 1 for axis in "cxyz")
    return pl.pallas_call(
        lambda *refs: back_kernel(sizes, rows, block, *refs),
        out_shape=[jax.ShapeDtypeStruct(shape, F32) for shape in shapes],
        in_specs=[pl.BlockSpec(memory_space=pltpu.SMEM)] + [vmem] * 14,
        out_specs=[vmem] * len(shapes),
        scratch_shapes=[
            pltpu.VMEM((rows, 256), BF16),
            pltpu.VMEM((2, 128, rows), BF16),
            pltpu.VMEM((rows, 256), F32),
            pltpu.VMEM((rows, 256), F32),
            pltpu.VMEM((rows, 256), F32),
            pltpu.VMEM((3, rows, 256), BF16),
            pltpu.VMEM((3, zs, ys, shard, 256), BF16),
            pltpu.VMEM((rows, 512), F32),
            pltpu.VMEM((2, zs, ys, shard, 1024), BF16),
            pltpu.VMEM((zs, ys, shard, 256), BF16),
            pltpu.VMEM((2, own, 512), F32),
            pltpu.VMEM((own, 512), BF16),
            pltpu.VMEM((own, 512), BF16),
            pltpu.VMEM((4, 40, 512), F32),
            pltpu.VMEM((meets, 40, 512), F32),
            pltpu.SemaphoreType.DMA((1,)),
            pltpu.SemaphoreType.DMA((slots,)),
            pltpu.SemaphoreType.DMA((slots,)),
            pltpu.SemaphoreType.DMA((6 + meets,)),
            pltpu.SemaphoreType.DMA((6 + meets,)),
        ]
        + [pltpu.VMEM(shape, BF16) for shape in lands],
        name="back",
        compiler_params=pltpu.CompilerParams(
            collective_id=1, has_side_effects=True, vmem_limit_bytes=VMEM_LIMIT
        ),
    )(lengths, grad_attended, q, k, v, lse, normed, qkv, grad_middle, x, gain, tables, grad_ff, grad_out, stats)


def solution(mesh):
    dp, tensor = mesh.shape["dp"], mesh.shape["tensor"]
    sizes = {"z": dp // 2, "y": 2, "x": tensor // 2, "c": 2}

    def shards(
        inputs, qkv_weight, out_weight, up_weight, down_weight, gain_one, shift_one, gain_two, shift_two, lengths,
        teacher, cotangent,
    ):
        own, sequences, width = inputs.shape
        rows = own * tensor
        shard = width // dp

        def packed(value):
            view = value.reshape(own, sequences, width // 128, 128).transpose(0, 2, 1, 3)
            return view.reshape(own * sequences * (width // 128), 128)

        def unpacked(value):
            view = value.reshape(own, width // 128, sequences, 128).transpose(0, 2, 1, 3)
            return view.reshape(own, sequences, width)

        x = packed(inputs)
        tables = rope_tables(rows)
        ff_all, out_all, qkv_all, counts, normed, q, k, v, lse, attended = front(
            sizes, rows, lengths, x, qkv_weight, out_weight.T, up_weight, down_weight.T, gain_one[None],
            shift_one[None], tables,
        )
        output, grad_middle, grad_attended, grad_ff, grad_out, stats = middle_part(
            own, float(rows * sequences * dp), lengths, counts.reshape(dp, 8, 128), x, packed(teacher),
            packed(cotangent), attended, ff_all.reshape(tensor, width, 1024), out_all.reshape(2, width, 256),
            gain_two[None], shift_two[None],
        )
        grad_inputs, up, down, out, qkv, sums = back(
            sizes, rows, lengths, grad_attended, q, k, v, lse, normed, qkv_all.reshape(3, width, 256), grad_middle, x,
            gain_one[None], tables, grad_ff.reshape(ff_all.shape), grad_out.reshape(out_all.shape), stats,
        )
        total = jnp.sum(counts[:, :, 0, 0])
        loss = jnp.sum(sums[0, :128]) / (total * width)
        return (
            unpacked(output), loss, unpacked(grad_inputs), qkv, out.T, up, down.T, sums[24], sums[32], sums[8], sums[16],
        )

    tokens, rows_dp, cols_dp = P("tensor", "dp", None), P("dp", "tensor"), P("tensor", "dp")
    heads = P(None, "dp", "tensor")
    return jax.shard_map(
        shards,
        mesh=mesh,
        in_specs=(tokens, heads, cols_dp, rows_dp, cols_dp, P(), P(), P(), P(), P("dp"), tokens, tokens),
        out_specs=(tokens, P(), tokens, heads, cols_dp, rows_dp, cols_dp, P(), P(), P(), P()),
        check_vma=False,
    )
```

```python
import math

import jax
import jax.numpy as jnp
import numpy as np
from jax import lax
from jax.experimental import pallas as pl
from jax.experimental.pallas import tpu as pltpu
from jax.sharding import PartitionSpec as P

HD = 64
F32 = jnp.float32
BF16 = jnp.bfloat16
MESH = pl.DeviceIdType.MESH
VMEM_LIMIT = 60 * 1024 * 1024

NN = (((1,), (0,)), ((), ()))
NT = (((1,), (1,)), ((), ()))


def dot(a, b, dims=NN):
    return lax.dot_general(a, b, dims, preferred_element_type=F32)


class Place:
    def __init__(self, sizes):
        dp, tensor = lax.axis_index("dp"), lax.axis_index("tensor")
        self.sizes = sizes
        self.at = {"z": dp // sizes["y"], "y": dp % sizes["y"], "x": tensor // 2, "c": tensor % 2}

    def moved(self, axis, delta):
        size = self.sizes[axis]
        if size == 2:
            return 1 - self.at[axis]
        return lax.rem(self.at[axis] + (delta % size), size)

    def device(self, **moves):
        at = dict(self.at)
        for axis, delta in moves.items():
            at[axis] = self.moved(axis, delta)
        return (at["z"] * self.sizes["y"] + at["y"], at["x"] * 2 + at["c"])

    def peers(self):
        out = [self.device(x=1), self.device(c=1), self.device(x=1, c=1), self.device(y=1)]
        out += [self.device(z=delta) for delta in range(1, self.sizes["z"])]
        return out

    def meet(self):
        barrier = pltpu.get_barrier_semaphore()
        peers = self.peers()
        for peer in peers:
            pl.semaphore_signal(barrier, inc=1, device_id=peer, device_id_type=MESH)
        return lambda: pl.semaphore_wait(barrier, len(peers))


def remote(src, dst, send, recv, device):
    return pltpu.make_async_remote_copy(
        src_ref=src, dst_ref=dst, send_sem=send, recv_sem=recv, device_id=device, device_id_type=MESH
    )


def steps_of(sizes, order):
    out = []
    for axis in order:
        out += ["z1", "z2"] if axis == "z" and sizes["z"] == 4 else [axis]
    return out


def slots_of(sizes, order):
    return sum(2 if step in ("z1", "z2") else sizes[step] - 1 for step in steps_of(sizes, order))


class Gather:
    def __init__(self, place, view, order, rows, send, recv, base):
        self.place, self.view, self.order = place, view, order
        self.send, self.recv, self.base = send, recv, base
        self.low, self.high = pl.ds(0, rows // 2), pl.ds(rows // 2, rows // 2)
        self.steps = steps_of(place.sizes, order)

    def part(self, step, **changed):
        where = dict(self.place.at)
        where["r"] = slice(None)
        for axis in self.order[: self.order.index(self.steps[step][0])]:
            where[axis] = slice(None)
        where.update(changed)
        return self.view(where)

    def copies(self, step):
        name, moved = self.steps[step], self.place.moved
        if name == "z1":
            return [(self.part(step), self.part(step, z=moved("z", -d)), {"z": d}) for d in (1, -1)]
        if name == "z2":
            out = []
            for d, rows in ((1, self.low), (-1, self.high)):
                far = self.part(step, z=moved("z", 2), r=rows)
                out.append((self.part(step, z=moved("z", -d), r=rows), far, {"z": d}))
            return out
        size = self.place.sizes[name]
        return [
            (self.part(step), self.part(step, **{name: moved(name, -d)}), {name: d}) for d in range(1, size)
        ]

    def made(self, step, came):
        slot = self.base
        for index in range(step):
            slot += len(self.copies(index))
        for source, landed, moves in self.copies(step):
            ref = landed if came else source
            yield remote(ref, ref, self.send.at[slot], self.recv.at[slot], self.place.device(**moves))
            slot += 1

    def start(self, step):
        for copy in self.made(step, False):
            copy.start()

    def arrive(self, step):
        for copy in self.made(step, True):
            copy.wait_recv()

    def next(self, step):
        if 0 < step <= len(self.steps):
            self.arrive(step - 1)
        if step < len(self.steps):
            self.start(step)

    def finish(self):
        for step in range(len(self.steps)):
            for copy in self.made(step, False):
                copy.wait_send()


def lanes(shape, limit):
    return lax.broadcasted_iota(jnp.int32, shape, 1) < limit


def token_rows(ref, seq, rows):
    return [ref[pl.ds(2 * j + seq, rows, stride=8), :] for j in range(4)]


def row_mean(parts):
    total = parts[0]
    for part in parts[1:]:
        total = total + part
    return jnp.sum(total, -1, keepdims=True) * (1.0 / (128 * len(parts)))


def normalize(parts):
    mean = row_mean(parts)
    center = [part - mean for part in parts]
    spread = row_mean([part * part for part in center])
    scale = lax.rsqrt(spread + 1e-05)
    return center, scale


def rope(value, cos, sin_a, sin_b):
    return value * cos + pltpu.roll(value, 96, 1) * sin_a + pltpu.roll(value, 32, 1) * sin_b


def rope_back(grad, cos, sin_a, sin_b):
    return grad * cos - pltpu.roll(grad, 96, 1) * sin_a - pltpu.roll(grad, 32, 1) * sin_b


def rope_tables(rows):
    half = HD // 2
    rates = np.exp(np.arange(half, dtype=np.float32) * np.float32(-2.0 * math.log(10000.0) / HD))
    angles = np.arange(rows, dtype=np.float32)[:, None] * rates.astype(np.float32)[None, :]
    cos, sin, zero = np.cos(angles), np.sin(angles), np.zeros_like(angles)
    tables = [[cos] * 4, [-sin, zero] * 2, [zero, sin] * 2]
    return jnp.asarray(np.stack([np.concatenate(table, -1) for table in tables]).astype(np.float32))


FRONT = (("q", "xzy"), ("k", "zyx"), ("v", "yxz"), ("n", "zy"), ("out", "xyzc"), ("u0", "xyzc"), ("u1", "xyzc"), ("d0", "xyzc"), ("d1", "zxyc"))


def x_lane(index):
    return index if isinstance(index, slice) else pl.ds(pl.multiple_of(index * 128, 128), 128)


def front_kernel(
    sizes,
    rows,
    block,
    lengths,
    x_ref,
    qkv_shard,
    out_shard,
    up_shard,
    down_shard,
    gain,
    shift,
    tables,
    ff_all,
    out_all,
    qkv_all,
    counts,
    normed_all,
    q_all,
    k_all,
    v_all,
    lse,
    attended,
    own_normed,
    own_attended,
    local_sem,
    send,
    recv,
    send_n,
    recv_n,
    send_a,
    recv_a,
):
    place = Place(sizes)
    at = place.at
    x, c, z, y = at["x"], at["c"], at["z"], at["y"]
    t = x * 2 + c
    own = rows // 4
    shard = qkv_shard.shape[1]
    met = place.meet()

    def local(index, src, dst):
        copy = pltpu.make_async_copy(src, dst, local_sem.at[index])
        copy.start()
        return copy

    def row_block(index):
        return pl.ds(pl.multiple_of(index * own, own), own)

    def qkv_view(i):
        return lambda w: qkv_all.at[i, w["z"], w["y"], w["r"], x_lane(w["x"])]

    def ff_view(start):
        return lambda w: ff_all.at[w["x"], w["c"], w["z"], w["y"], w["r"], pl.ds(start, 256)]

    views = {
        "q": qkv_view(0),
        "k": qkv_view(1),
        "v": qkv_view(2),
        "n": lambda w: counts.at[w["z"], w["y"], w["r"]],
        "out": lambda w: out_all.at[w["c"], w["z"], w["y"], w["r"], x_lane(w["x"])],
        "u0": ff_view(0),
        "u1": ff_view(256),
        "d0": ff_view(512),
        "d1": ff_view(768),
    }
    plans = {}
    base = 0
    for name, order in FRONT:
        plans[name] = Gather(place, views[name], order, 16 if name == "n" else shard, send, recv, base)
        base += slots_of(sizes, order)

    def go(names, step):
        for name in names:
            plans[name].next(step)

    copies = [
        local(0, qkv_shard, qkv_all.at[:, z, y, :, x_lane(x)]),
        local(1, out_shard, out_all.at[c, z, y, :, x_lane(x)]),
        local(2, up_shard, ff_all.at[x, c, z, y, :, pl.ds(0, 512)]),
        local(3, down_shard, ff_all.at[x, c, z, y, :, pl.ds(512, 512)]),
    ]
    total = lengths[0] + lengths[1]
    counts[z, y] = jnp.full((16, 128), total.astype(F32))
    copies[0].wait()
    met()
    heads, ff = ("q", "k", "v"), ("u0", "d0", "out", "u1", "d1")
    go(heads, 0)
    go("n", 0)
    for s in range(2):
        center, scale = normalize(token_rows(x_ref, s, own))
        for j in range(4):
            lane = pl.ds(128 * j, 128)
            value = center[j] * scale * gain[:, lane] + shift[:, lane]
            own_normed[s, :, lane] = value.astype(BF16)
    mine = row_block(t)

    def tokens(index, ref, moves):
        return remote(ref, ref, send_n.at[index], recv_n.at[index], place.device(**moves))

    sent = [
        remote(own_normed.at[1 - x], normed_all.at[mine], send_n.at[0], recv_n.at[0], place.device(x=1)),
        remote(own_normed.at[x], normed_all.at[mine], send_n.at[1], recv_n.at[1], place.device(c=1)),
    ]
    for copy in sent:
        copy.start()
    keep = local(0, own_normed.at[x], normed_all.at[mine])
    for copy in copies[1:]:
        copy.wait()
    go(heads, 1)
    go("n", 1)
    go(ff, 0)
    go(heads, 2)
    go(ff[:2], 1)
    far = normed_all.at[row_block((1 - x) * 2 + c)]
    tokens(0, far, {"x": 1}).wait_recv()
    sent.append(tokens(2, far, {"c": 1}))
    sent[-1].start()
    go(heads, 3)
    go("n", 2)
    go(ff[2:], 1)
    keep.wait()
    tokens(1, normed_all.at[row_block(x * 2 + 1 - c)], {"c": 1}).wait_recv()
    go(heads, 4)
    tokens(2, normed_all.at[row_block((1 - x) * 2 + 1 - c)], {"c": 1}).wait_recv()
    go(ff, 2)

    w_qkv = [qkv_all[i].reshape(-1, 256) for i in range(3)]

    def project(index, carry):
        here = pl.ds(pl.multiple_of(index * block, block), block)
        normed = normed_all[here, :]
        cos, sin_a, sin_b = (tables[i, here, :] for i in range(3))
        for i, ref in ((0, q_all), (1, k_all), (2, v_all)):
            value = dot(normed, w_qkv[i])
            for pair in range(2):
                lane = pl.ds(128 * pair, 128)
                part = value[:, 128 * pair : 128 * pair + 128]
                if i < 2:
                    part = rope(part, cos, sin_a, sin_b)
                if i == 0:
                    part = part.astype(BF16) * jnp.asarray(HD**-0.5, BF16)
                ref[here, lane] = part.astype(BF16)
        return carry

    lax.fori_loop(0, rows // block, project, 0)
    go("n", 3)
    go(ff[:2], 3)

    length = lengths[x]
    half = lanes((block, 128), HD)
    zero = jnp.zeros((block, 128), BF16)
    blocks = rows // block

    def hand(qb, act):
        to = {"x": qb // 2, "c": qb % 2}
        source, target = own_attended.at[pl.ds(qb * block, block)], attended.at[c, x]
        device = (lax.axis_index("dp"), jnp.asarray(qb, jnp.int32))

        @pl.when(t != qb)
        def _():
            copy = remote(source, target, send_a.at[qb], recv_a.at[t], device)
            if act == "start":
                copy.start()
            else:
                copy.wait_send()

        if act == "start":

            @pl.when(t == qb)
            def _():
                pltpu.make_async_copy(source, target, recv_a.at[t]).start()

    for qb in range(blocks):
        here = pl.ds(qb * block, block)
        keys = (qb + 1) * block
        key_pos = lax.broadcasted_iota(jnp.int32, (block, keys), 1)
        query_pos = lax.broadcasted_iota(jnp.int32, (block, keys), 0) + qb * block
        allowed = key_pos <= query_pos
        if keys > rows // 2:
            allowed = allowed & (key_pos < length)

        def attend(pair, carry, here=here, keys=keys, allowed=allowed):
            lane = pl.ds(pl.multiple_of(pair * 128, 128), 128)
            queries = q_all[here, lane]
            k_part = k_all[pl.ds(0, keys), lane]
            v_part = v_all[pl.ds(0, keys), lane]
            mixed = []
            for head in range(2):
                masked = jnp.where(half, queries, zero) if head == 0 else jnp.where(half, zero, queries)
                scores = jnp.where(allowed, dot(masked, k_part, NT), -1e30)
                highest = jnp.max(scores, -1, keepdims=True)
                expd = jnp.exp(scores - highest)
                denom = jnp.sum(expd, -1, keepdims=True)
                probs = (expd * (1.0 / denom)).astype(BF16)
                mixed.append(dot(probs, v_part))
                wide = jnp.broadcast_to(highest + jnp.log(denom), (block, 128))
                lse[pair * 2 + head, :, here] = jnp.transpose(wide)[:8]
            own_attended[here, lane] = jnp.where(half, mixed[0], mixed[1]).astype(BF16)
            return carry

        lax.fori_loop(0, 2, attend, 0)
        hand(qb, "start")
        if qb == 1:
            go(ff[2:], 3)
        if qb == 2:
            go(ff[:2], 4)
    go(ff[2:], 4)
    for k in range(2):
        for s in range(2):
            came = attended.at[k, s]
            index = s * 2 + k
            remote(came, came, send_a.at[0], recv_a.at[index], place.device(x=1)).wait_recv()
    go(ff, 5)
    for plan in plans.values():
        plan.finish()
    for copy in sent:
        copy.wait_send()
    for qb in range(blocks):
        hand(qb, "finish")


def front(sizes, rows, lengths, x, qkv, out, up, down, gain, shift, tables):
    zs, ys = sizes["z"], sizes["y"]
    shard = qkv.shape[1]
    own = rows // 4
    slots = sum(slots_of(sizes, order) for _, order in FRONT)
    any_spec = pl.BlockSpec(memory_space=pl.ANY)
    vmem = pl.BlockSpec(memory_space=pltpu.VMEM)
    shapes = [
        ((2, 2, zs, ys, shard, 1024), BF16),
        ((2, zs, ys, shard, 256), BF16),
        ((3, zs, ys, shard, 256), BF16),
        ((zs, ys, 16, 128), F32),
        ((rows, 512), BF16),
        ((rows, 256), BF16),
        ((rows, 256), BF16),
        ((rows, 256), BF16),
        ((4, 8, rows), F32),
        ((2, 2, own, 256), BF16),
    ]
    return pl.pallas_call(
        lambda *refs: front_kernel(sizes, rows, own, *refs),
        out_shape=[jax.ShapeDtypeStruct(*shape) for shape in shapes],
        in_specs=[pl.BlockSpec(memory_space=pltpu.SMEM), vmem] + [any_spec] * 4 + [vmem] * 3,
        out_specs=[vmem] * len(shapes),
        scratch_shapes=[
            pltpu.VMEM((2, own, 512), BF16),
            pltpu.VMEM((rows, 256), BF16),
            pltpu.SemaphoreType.DMA((4,)),
            pltpu.SemaphoreType.DMA((slots,)),
            pltpu.SemaphoreType.DMA((slots,)),
            pltpu.SemaphoreType.DMA((3,)),
            pltpu.SemaphoreType.DMA((3,)),
            pltpu.SemaphoreType.DMA((4,)),
            pltpu.SemaphoreType.DMA((4,)),
        ],
        name="front",
        compiler_params=pltpu.CompilerParams(
            collective_id=0, has_side_effects=True, vmem_limit_bytes=VMEM_LIMIT
        ),
    )(lengths, x, qkv, out, up, down, gain, shift, tables)


def gelu_parts(value):
    cdf = 0.5 + 0.5 * lax.erf(value * (2.0**-0.5))
    density = jnp.exp(-0.5 * value * value) * ((2.0 * math.pi) ** -0.5)
    return value * cdf, cdf + value * density


def middle_kernel(
    own,
    tensor_total,
    lengths,
    counts,
    x_ref,
    teacher,
    cotangent,
    attended,
    ff_all,
    out_all,
    gain,
    shift,
    output,
    grad_middle,
    grad_attended,
    grad_ff,
    grad_out,
    stats,
    middle,
    seed,
    slope,
    hidden,
    total_sum,
):
    tokens = 2 * own
    tensor = lax.axis_index("tensor")
    count = jnp.sum(counts[...], axis=0)[0:1]
    factor = tensor_total / count
    valid = []
    for s in range(2):
        rows = pl.ds(s * own, own)
        attn = dot(attended[0, s], out_all[0], NT) + dot(attended[1, s], out_all[1], NT)
        parts = token_rows(x_ref, s, own)
        for j in range(4):
            middle[rows, pl.ds(128 * j, 128)] = parts[j] + attn[:, 128 * j : 128 * j + 128]
        position = tensor * own + lax.broadcasted_iota(jnp.int32, (own, 128), 0)
        valid.append((position < lengths[s]).astype(F32))
    value = middle[...]
    mean = jnp.mean(value, -1, keepdims=True)
    center = value - mean
    scale = lax.rsqrt(jnp.mean(center * center, -1, keepdims=True) + 1e-05)
    normed = (center * scale * gain[...] + shift[...]).astype(BF16)
    normed_t = jnp.transpose(normed)

    total_sum[...] = jnp.zeros_like(total_sum)

    def up(t, carry):
        before = dot(normed, ff_all[t, :, pl.ds(0, 512)])
        act, slope_t = gelu_parts(before)
        act = act.astype(BF16)
        slope[t] = slope_t
        hidden[t] = act
        total_sum[...] += dot(act, ff_all[t, :, pl.ds(512, 512)], NT)
        return carry

    lax.fori_loop(0, 4, up, 0)

    square = jnp.zeros((own, 128), F32)
    for s in range(2):
        rows = pl.ds(s * own, own)
        want = token_rows(teacher, s, own)
        weight = token_rows(cotangent, s, own)
        for j in range(4):
            lane = pl.ds(128 * j, 128)
            out = middle[rows, lane] + total_sum[rows, lane]
            output[pl.ds(2 * j + s, own, stride=8), :] = out
            differ = out - want[j]
            square = square + valid[s] * differ * differ
            seed[rows, lane] = factor * valid[s] * (weight[j] + differ)
    grad_f = seed[...].astype(BF16)
    grad_f_t = jnp.transpose(grad_f)
    total_sum[...] = jnp.zeros_like(total_sum)

    def down(t, carry):
        grad_hidden = dot(grad_f, ff_all[t, :, pl.ds(512, 512)])
        grad_before = (slope[t] * grad_hidden).astype(BF16)
        grad_ff[t, :, pl.ds(0, 512)] = dot(normed_t, grad_before).astype(BF16)
        grad_ff[t, :, pl.ds(512, 512)] = dot(grad_f_t, hidden[t]).astype(BF16)
        total_sum[...] += dot(grad_before, ff_all[t, :, pl.ds(0, 512)], NT)
        return carry

    lax.fori_loop(0, 4, down, 0)

    grad_normed = total_sum[...]
    unit = (middle[...] - mean) * scale
    stats[...] = jnp.zeros_like(stats)
    stats[0:1, 0:128] = jnp.sum(square, 0, keepdims=True)
    stats[8:9] = jnp.sum(grad_normed * unit, 0, keepdims=True)
    stats[16:17] = jnp.sum(grad_normed, 0, keepdims=True)
    scaled = grad_normed * gain[...]
    inner = jnp.mean(scaled * unit, -1, keepdims=True)
    grad = seed[...] + scale * (scaled - jnp.mean(scaled, -1, keepdims=True) - unit * inner)
    grad_middle[...] = grad
    branch = grad.astype(BF16)
    branch_t = jnp.transpose(branch)
    for k in range(2):
        grad_out[k] = (dot(branch_t[:, :own], attended[k, 0]) + dot(branch_t[:, own:], attended[k, 1])).astype(BF16)
        back = dot(branch, out_all[k]).astype(BF16)
        for s in range(2):
            grad_attended[k, s] = back[s * own : s * own + own]


def middle_part(own, tensor_total, lengths, counts, x, teacher, cotangent, attended, ff_all, out_all, gain, shift):
    tokens = 2 * own
    vmem = pl.BlockSpec(memory_space=pltpu.VMEM)
    shapes = [
        (x.shape, F32),
        ((tokens, 512), F32),
        ((2, 2, own, 256), BF16),
        ((4, 512, 1024), BF16),
        ((2, 512, 256), BF16),
        ((24, 512), F32),
    ]
    return pl.pallas_call(
        lambda *refs: middle_kernel(own, tensor_total, *refs),
        out_shape=[jax.ShapeDtypeStruct(*shape) for shape in shapes],
        in_specs=[pl.BlockSpec(memory_space=pltpu.SMEM)] + [vmem] * 9,
        out_specs=[vmem] * len(shapes),
        scratch_shapes=[
            pltpu.VMEM((tokens, 512), F32),
            pltpu.VMEM((tokens, 512), F32),
            pltpu.VMEM((4, tokens, 512), F32),
            pltpu.VMEM((4, tokens, 512), BF16),
            pltpu.VMEM((tokens, 512), F32),
        ],
        name="middle",
        compiler_params=pltpu.CompilerParams(vmem_limit_bytes=VMEM_LIMIT),
    )(lengths, counts, x, teacher, cotangent, attended, ff_all, out_all, gain, shift)


class Scatter:
    def __init__(self, place, view, work, order, dims, rows, lead, landing, final, send, recv, base):
        self.place, self.view, self.work, self.order, self.dims = place, view, work, order, dims
        self.lead, self.landing, self.final = lead, landing, final
        self.send, self.recv, self.base = send, recv, base
        self.low, self.high = pl.ds(0, rows // 2), pl.ds(rows // 2, rows // 2)
        self.steps = steps_of(place.sizes, order)

    def done(self, step):
        return self.order[: self.order.index(self.steps[step][0])]

    def part(self, step, kept=False, **changed):
        where = dict(self.place.at)
        where["r"] = slice(None)
        for axis in self.order:
            if axis not in self.done(step):
                where[axis] = slice(None)
        where.update(changed)
        return (self.work if kept or step > 0 else self.view)(where)

    def sends(self, step):
        name, moved = self.steps[step], self.place.moved
        if name == "z1":
            return [({"z": moved("z", 2), "r": rows}, {"z": d}) for d, rows in ((1, self.low), (-1, self.high))]
        if name == "z2":
            return [({"z": moved("z", d)}, {"z": d}) for d in (1, -1)]
        return [({name: moved(name, d)}, {name: d}) for d in range(1, self.place.sizes[name])]

    def sums(self, step):
        name, moved = self.steps[step], self.place.moved
        if name == "z1":
            return [({"z": moved("z", 1), "r": self.low}, [0]), ({"z": moved("z", -1), "r": self.high}, [1])]
        return [({name[0]: self.place.at[name[0]]}, list(range(len(self.sends(step)))))]

    def made(self, step):
        slot = self.base
        for index in range(step):
            slot += len(self.sends(index))
        for index, (where, moves) in enumerate(self.sends(step)):
            yield remote(
                self.part(step, **where),
                self.landing[step].at[index],
                self.send.at[slot + index],
                self.recv.at[slot + index],
                self.place.device(**moves),
            )

    def start(self, step):
        for copy in self.made(step):
            copy.start()

    def arrive(self, step):
        for copy in self.made(step):
            copy.wait_recv()
        axis = self.steps[step][0]
        rest = [a for a in self.dims if a in self.order and a not in self.done(step) and a != axis]
        sizes = [self.place.sizes[a] for a in rest]
        landing = self.landing[step]
        last = step == len(self.steps) - 1
        for where, pieces in self.sums(step):

            def add(index, carry, where=where, pieces=pieces):
                chosen = {}
                for a, size in zip(reversed(rest), reversed(sizes)):
                    chosen[a] = lax.rem(index, size)
                    index = index // size
                total = self.part(step, **chosen, **where)[...].astype(F32)
                for piece in pieces:
                    place = (piece,) + (slice(None),) * self.lead + tuple(chosen[a] for a in rest)
                    total = total + landing[place].astype(F32)
                if last:
                    self.final[...] = total
                else:
                    self.part(step, kept=True, **chosen, **where)[...] = total.astype(BF16)
                return carry

            count = math.prod(sizes)
            if count == 1:
                add(0, 0)
            else:
                lax.fori_loop(0, count, add, 0)

    def next(self, step):
        if 0 < step <= len(self.steps):
            self.arrive(step - 1)
        if step < len(self.steps):
            self.start(step)

    def finish(self):
        for step in range(len(self.steps)):
            for copy in self.made(step):
                copy.wait_send()


def landing_shapes(sizes, order, dims, rows, width, lead=(), lane_x=False):
    left = list(order)
    shapes = []
    for step in steps_of(sizes, order):
        axis = step[0]
        if step != "z2" and axis in left:
            left.remove(axis)
        count = 2 if step in ("z1", "z2") else sizes[axis] - 1
        high = rows // 2 if step == "z1" else rows
        wide = width * 2 if lane_x and "x" in left else width
        shapes.append((count,) + lead + tuple(sizes[a] for a in dims if a in left) + (high, wide))
    return shapes


BACK = (
    ("u0", "czyx", "xczy", 256, False),
    ("u1", "czyx", "xczy", 256, False),
    ("d0", "czyx", "xczy", 256, False),
    ("d1", "cyxz", "xczy", 256, False),
    ("out", "czyx", "czy", 128, True),
    ("q", "yzx", "zy", 128, True),
    ("k", "xyz", "zy", 128, True),
    ("v", "zxy", "zy", 128, True),
)


def back_kernel(
    sizes,
    rows,
    block,
    shard,
    lengths,
    grad_attended,
    q_all,
    k_all,
    v_all,
    lse,
    normed_all,
    qkv_all,
    grad_middle,
    x_ref,
    gain,
    tables,
    grad_ff,
    grad_out,
    stats,
    grad_inputs,
    up_final,
    down_final,
    out_final,
    qkv_final,
    stats_final,
    g_all,
    k_t,
    grad_q,
    grad_k,
    grad_v,
    grad_proj,
    grad_qkv,
    grad_n,
    ff_work,
    out_work,
    from_core,
    to_x,
    from_x,
    stat_send,
    stat_land,
    send,
    recv,
    send_g,
    recv_g,
    send_n,
    recv_n,
    send_s,
    recv_s,
    *landing,
):
    place = Place(sizes)
    at = place.at
    x, c, z, y = at["x"], at["c"], at["z"], at["y"]
    t = x * 2 + c
    own = rows // 4
    blocks = rows // block
    met = place.meet()

    def row_block(index):
        return pl.ds(pl.multiple_of(index * own, own), own)

    def ff_view(start):
        return lambda w: grad_ff.at[w["x"], w["c"], w["z"], w["y"], w["r"], pl.ds(start, 256)]

    def ff_kept(start):
        return lambda w: ff_work.at[w["x"], w["z"], w["y"], w["r"], pl.ds(start, 256)]

    def qkv_view(i):
        return lambda w: grad_qkv.at[i, w["z"], w["y"], w["r"], x_lane(w["x"])]

    views = {
        "u0": (ff_view(0), ff_kept(0), up_final.at[:, pl.ds(0, 256)]),
        "u1": (ff_view(256), ff_kept(256), up_final.at[:, pl.ds(256, 256)]),
        "d0": (ff_view(512), ff_kept(512), down_final.at[:, pl.ds(0, 256)]),
        "d1": (ff_view(768), ff_kept(768), down_final.at[:, pl.ds(256, 256)]),
        "out": (
            lambda w: grad_out.at[w["c"], w["z"], w["y"], w["r"], x_lane(w["x"])],
            lambda w: out_work.at[w["z"], w["y"], w["r"], x_lane(w["x"])],
            out_final,
        ),
    }
    for i, name in enumerate("qkv"):
        views[name] = (qkv_view(i), qkv_view(i), qkv_final.at[i])
    plans = {}
    base = 0
    used = 0
    for name, order, dims, width, lane_x in BACK:
        view, kept, final = views[name]
        count = len(steps_of(sizes, order))
        plans[name] = Scatter(
            place, view, kept, order, dims, shard, 0, landing[used : used + count], final, send, recv, base
        )
        used += count
        base += slots_of(sizes, order)

    def go(names, step):
        for name in names:
            plans[name].next(step)

    met()
    moved = []
    for moves in ({"x": 1}, {"x": 1, "c": 1}, {"c": 1}):
        to = dict(at)
        for axis in moves:
            to[axis] = 1 - at[axis]
        copy = remote(
            grad_attended.at[to["c"], to["x"]],
            g_all.at[row_block(t)],
            send_g.at[len(moved)],
            recv_g.at[t],
            place.device(**moves),
        )
        copy.start()
        moved.append(copy)
    pltpu.make_async_copy(grad_attended.at[c, x], g_all.at[row_block(t)], recv_g.at[t]).start()
    ff = ("u0", "d0", "u1", "d1", "out")
    go(ff, 0)
    for pair in range(2):
        k_t[pair] = jnp.transpose(k_all[:, pl.ds(128 * pair, 128)])
    normed_t = jnp.transpose(normed_all[...])
    go(ff[:2], 1)

    length = lengths[x]
    half = lanes((block, 128), HD)
    zero = jnp.zeros((block, 128), BF16)
    upper = lax.broadcasted_iota(jnp.int32, (128, block), 0) < HD

    def to_core(qb, act):
        @pl.when(c != qb % 2)
        def _():
            copy = remote(
                grad_n.at[pl.ds(qb * block, block)],
                from_core.at[qb // 2],
                send_n.at[qb // 2],
                recv_n.at[qb // 2],
                place.device(c=1),
            )
            copy.start() if act == "start" else copy.wait_send()

    def arrived(index):
        slot = from_core.at[index]
        remote(slot, slot, send_n.at[index], recv_n.at[index], place.device(c=1)).wait_recv()

    def cross():
        return remote(to_x, from_x, send_n.at[2], recv_n.at[2], place.device(x=1))

    def to_chip(qb):
        @pl.when((c == qb % 2) & (x != qb // 2))
        def _():
            arrived(qb // 2)
            to_x[...] = (grad_n[pl.ds(qb * block, block), :] + from_core[qb // 2]).astype(BF16)
            cross().start()

    for qb in range(blocks - 1, -1, -1):
        here = pl.ds(qb * block, block)
        keys = (qb + 1) * block
        seen = pl.ds(0, keys)
        key_pos = lax.broadcasted_iota(jnp.int32, (keys, block), 0)
        query_pos = lax.broadcasted_iota(jnp.int32, (keys, block), 1) + qb * block
        allowed = key_pos <= query_pos
        if keys > rows // 2:
            allowed = allowed & (key_pos < length)
        came = g_all.at[here]
        remote(came, came, send_g.at[0], recv_g.at[qb], place.device(x=1)).wait_recv()

        def attend(pair, carry, qb=qb, here=here, seen=seen, keys=keys, allowed=allowed):
            lane = pl.ds(pl.multiple_of(pair * 128, 128), 128)
            queries = q_all[here, lane]
            grads = g_all[here, lane]
            k_part = k_all[seen, lane]
            v_part = v_all[seen, lane]
            dq = []
            for head in range(2):
                if head == 0:
                    q_m, g_m = jnp.where(half, queries, zero), jnp.where(half, grads, zero)
                else:
                    q_m, g_m = jnp.where(half, zero, queries), jnp.where(half, zero, grads)
                scores = dot(k_part, q_m, NT)
                probs = jnp.where(allowed, jnp.exp(scores - lse[pair * 2 + head, 0:1, here]), 0.0)
                grad_probs = dot(v_part, g_m, NT)
                inner = jnp.sum(probs * grad_probs, 0, keepdims=True)
                grad_raw = (probs * (grad_probs - inner)).astype(BF16)
                add_k = dot(grad_raw, q_m)
                add_v = dot(probs.astype(BF16), g_m)
                if qb == blocks - 1 and head == 0:
                    grad_k[seen, lane] = add_k
                    grad_v[seen, lane] = add_v
                else:
                    grad_k[seen, lane] += add_k
                    grad_v[seen, lane] += add_v
                dq.append(dot(k_t[pair, :, seen], grad_raw))
            grad_q[here, lane] = jnp.transpose(jnp.where(upper, dq[0], dq[1])) * HD**-0.5
            return carry

        lax.fori_loop(0, 2, attend, 0)

        cos, sin_a, sin_b = (tables[i, here, :] for i in range(3))
        total = jnp.zeros((block, 512), F32)
        for i, ref in ((0, grad_q), (1, grad_k), (2, grad_v)):
            for pair in range(2):
                lane = pl.ds(128 * pair, 128)
                part = ref[here, lane]
                if i < 2:
                    part = rope_back(part, cos, sin_a, sin_b)
                grad_proj[i, here, lane] = part.astype(BF16)
            total = total + dot(grad_proj[i, here, :], qkv_all[i], NT)
        grad_n[here, :] = total
        to_core(qb, "start")
        if qb < blocks - 1:
            to_chip(qb + 1)
        if qb == blocks - 1:
            go(ff[2:], 1)
            go(ff[:2], 2)
        if qb == blocks - 2:
            go(ff[2:], 2)
            go(ff[:2], 3)
        if qb == blocks - 3:
            go(ff[2:], 3)
            go(ff[:2], 4)
    deep = sizes["z"] * sizes["y"]
    for i, name in enumerate("qkv"):
        value = dot(normed_t, grad_proj[i]).astype(BF16)
        grad_qkv[i] = value.reshape(sizes["z"], sizes["y"], shard, 256)
        go(name, 0)
        if i == 0:
            to_chip(0)
    go(ff[2:], 4)
    go(ff[:2], 5)
    stat_send[0] = jnp.zeros_like(stat_send[0])
    stat_send[0, 0:24] = stats[...]
    arrived_own = x
    slot = from_core.at[arrived_own]
    remote(slot, slot, send_n.at[0], recv_n.at[arrived_own], place.device(c=1)).wait_recv()
    cross().wait_recv()
    go("qkv", 1)
    grad_gain = [jnp.zeros((1, 128), F32)] * 4
    grad_shift = [jnp.zeros((1, 128), F32)] * 4
    for s in range(2):
        center, scale = normalize(token_rows(x_ref, s, own))
        near = grad_n[row_block(t), :] + from_core[x]
        chosen = jnp.where(x == s, near, from_x[...].astype(F32))
        grads = [chosen[:, 128 * j : 128 * j + 128] for j in range(4)]
        units = [part * scale for part in center]
        scaled = [grads[j] * gain[:, pl.ds(128 * j, 128)] for j in range(4)]
        mean = row_mean(scaled)
        inner = row_mean([scaled[j] * units[j] for j in range(4)])
        for j in range(4):
            part = grad_middle[pl.ds(s * own, own), pl.ds(128 * j, 128)]
            grad_inputs[pl.ds(2 * j + s, own, stride=8), :] = part + scale * (scaled[j] - mean - units[j] * inner)
            grad_gain[j] = grad_gain[j] + jnp.sum(grads[j] * units[j], 0, keepdims=True)
            grad_shift[j] = grad_shift[j] + jnp.sum(grads[j], 0, keepdims=True)
    for j in range(4):
        stat_send[0, 24:25, 128 * j : 128 * j + 128] = grad_gain[j]
        stat_send[0, 32:33, 128 * j : 128 * j + 128] = grad_shift[j]

    slot = 0
    stat_sent = []
    for phase, axis in enumerate("cxyz"):
        came = []
        for delta in range(1, sizes[axis]):
            copy = remote(
                stat_send.at[phase], stat_land.at[slot], send_s.at[slot], recv_s.at[slot], place.device(**{axis: delta})
            )
            copy.start()
            came.append((copy, slot))
            stat_sent.append(copy)
            slot += 1
        if phase + 2 <= len(plans["q"].steps):
            go("qkv", phase + 2)
        if phase == 1:
            go(ff[2:], 5)
        total = stat_send[phase]
        for copy, index in came:
            copy.wait_recv()
            total = total + stat_land[index]
        if phase < 3:
            stat_send[phase + 1] = total
        else:
            stats_final[...] = total
    for plan in plans.values():
        plan.finish()
    for copy in moved + [cross()] + stat_sent:
        copy.wait_send()
    for qb in range(blocks):
        to_core(qb, "finish")


def back(sizes, rows, lengths, grad_attended, q, k, v, lse, normed, qkv, grad_middle, x, gain, tables, grad_ff, grad_out, stats):
    zs, ys = sizes["z"], sizes["y"]
    shard = 512 // (zs * ys)
    own = rows // 4
    vmem = pl.BlockSpec(memory_space=pltpu.VMEM)
    shapes = [x.shape, (shard, 512), (shard, 512), (shard, 128), (3, shard, 128), (40, 512)]
    lands = []
    for _, order, dims, width, lane_x in BACK:
        lands += landing_shapes(sizes, order, dims, shard, width, lane_x=lane_x)
    slots = sum(slots_of(sizes, item[1]) for item in BACK)
    meets = sum(sizes[axis] - 1 for axis in "cxyz")
    return pl.pallas_call(
        lambda *refs: back_kernel(sizes, rows, own, shard, *refs),
        out_shape=[jax.ShapeDtypeStruct(shape, F32) for shape in shapes],
        in_specs=[pl.BlockSpec(memory_space=pltpu.SMEM)] + [vmem] * 14,
        out_specs=[vmem] * len(shapes),
        scratch_shapes=[
            pltpu.VMEM((rows, 256), BF16),
            pltpu.VMEM((2, 128, rows), BF16),
            pltpu.VMEM((rows, 256), F32),
            pltpu.VMEM((rows, 256), F32),
            pltpu.VMEM((rows, 256), F32),
            pltpu.VMEM((3, rows, 256), BF16),
            pltpu.VMEM((3, zs, ys, shard, 256), BF16),
            pltpu.VMEM((rows, 512), F32),
            pltpu.VMEM((2, zs, ys, shard, 1024), BF16),
            pltpu.VMEM((zs, ys, shard, 256), BF16),
            pltpu.VMEM((2, own, 512), F32),
            pltpu.VMEM((own, 512), BF16),
            pltpu.VMEM((own, 512), BF16),
            pltpu.VMEM((4, 40, 512), F32),
            pltpu.VMEM((meets, 40, 512), F32),
            pltpu.SemaphoreType.DMA((slots,)),
            pltpu.SemaphoreType.DMA((slots,)),
            pltpu.SemaphoreType.DMA((3,)),
            pltpu.SemaphoreType.DMA((4,)),
            pltpu.SemaphoreType.DMA((3,)),
            pltpu.SemaphoreType.DMA((3,)),
            pltpu.SemaphoreType.DMA((meets,)),
            pltpu.SemaphoreType.DMA((meets,)),
        ]
        + [pltpu.VMEM(shape, BF16) for shape in lands],
        name="back",
        compiler_params=pltpu.CompilerParams(
            collective_id=1, has_side_effects=True, vmem_limit_bytes=VMEM_LIMIT
        ),
    )(lengths, grad_attended, q, k, v, lse, normed, qkv, grad_middle, x, gain, tables, grad_ff, grad_out, stats)


def last_kernel(features, counts, grad_inputs, up, down, out, qkv, sums, *outs):
    for source, target in zip((grad_inputs, up, down, out, qkv), outs[:5]):
        target[...] = source[...]
    for target, row in zip(outs[5:9], (24, 32, 8, 16)):
        target[...] = sums[row : row + 1]
    total = jnp.sum(counts[...], axis=0)[0:1, 0:1]
    outs[9][...] = jnp.sum(sums[0:1, 0:128], -1, keepdims=True) / (total * features)


def last(features, counts, grad_inputs, up, down, out, qkv, sums):
    vmem = pl.BlockSpec(memory_space=pltpu.VMEM)
    shapes = [value.shape for value in (grad_inputs, up, down, out, qkv)] + [(1, features)] * 4 + [(1, 1)]
    return pl.pallas_call(
        lambda *refs: last_kernel(features, *refs),
        out_shape=[jax.ShapeDtypeStruct(shape, F32) for shape in shapes],
        in_specs=[vmem] * 7,
        out_specs=[vmem] * len(shapes),
        name="last",
        compiler_params=pltpu.CompilerParams(vmem_limit_bytes=VMEM_LIMIT),
    )(counts, grad_inputs, up, down, out, qkv, sums)


def solution(mesh):
    dp, tensor = mesh.shape["dp"], mesh.shape["tensor"]
    sizes = {"z": dp // 2, "y": 2, "x": tensor // 2, "c": 2}

    def shards(
        inputs, qkv_weight, out_weight, up_weight, down_weight, gain_one, shift_one, gain_two, shift_two, lengths,
        teacher, cotangent,
    ):
        own, sequences, width = inputs.shape
        rows = own * tensor
        shard = width // dp

        def packed(value):
            view = value.reshape(own, sequences, width // 128, 128).transpose(0, 2, 1, 3)
            return view.reshape(own * sequences * (width // 128), 128)

        def unpacked(value):
            view = value.reshape(own, width // 128, sequences, 128).transpose(0, 2, 1, 3)
            return view.reshape(own, sequences, width)

        x = packed(inputs)
        tables = rope_tables(rows)
        ff_all, out_all, qkv_all, counts, normed, q, k, v, lse, attended = front(
            sizes, rows, lengths, x, qkv_weight, out_weight.T, up_weight, down_weight.T, gain_one[None],
            shift_one[None], tables,
        )
        output, grad_middle, grad_attended, grad_ff, grad_out, stats = middle_part(
            own, float(rows * sequences * dp), lengths, counts.reshape(dp, 16, 128), x, packed(teacher),
            packed(cotangent), attended, ff_all.reshape(tensor, width, 1024), out_all.reshape(2, width, 256),
            gain_two[None], shift_two[None],
        )
        grad_inputs, up, down, out, qkv, sums = back(
            sizes, rows, lengths, grad_attended, q, k, v, lse, normed, qkv_all.reshape(3, width, 256), grad_middle, x,
            gain_one[None], tables, grad_ff.reshape(ff_all.shape), grad_out.reshape(out_all.shape), stats,
        )
        grad_inputs, up, down, out, qkv, gain_1, shift_1, gain_2, shift_2, loss = last(
            width, counts.reshape(dp, 16, 128), grad_inputs, up, down, out, qkv, sums
        )
        return (
            unpacked(output), loss.reshape(()), unpacked(grad_inputs), qkv, out.T, up, down.T, gain_1.reshape(width),
            shift_1.reshape(width), gain_2.reshape(width), shift_2.reshape(width),
        )

    tokens, rows_dp, cols_dp = P("tensor", "dp", None), P("dp", "tensor"), P("tensor", "dp")
    heads = P(None, "dp", "tensor")
    return jax.shard_map(
        shards,
        mesh=mesh,
        in_specs=(tokens, heads, cols_dp, rows_dp, cols_dp, P(), P(), P(), P(), P("dp"), tokens, tokens),
        out_specs=(tokens, P(), tokens, heads, cols_dp, rows_dp, cols_dp, P(), P(), P(), P()),
        check_vma=False,
    )
```

```python
import math

import jax
import jax.numpy as jnp
import numpy as np
from jax import lax
from jax.experimental import pallas as pl
from jax.experimental.pallas import tpu as pltpu
from jax.sharding import PartitionSpec as P

HD = 64
F32 = jnp.float32
BF16 = jnp.bfloat16
MESH = pl.DeviceIdType.MESH
VMEM_LIMIT = 60 * 1024 * 1024

NN = (((1,), (0,)), ((), ()))
NT = (((1,), (1,)), ((), ()))


def dot(a, b, dims=NN):
    return lax.dot_general(a, b, dims, preferred_element_type=F32)


class Place:
    def __init__(self, sizes):
        dp, tensor = lax.axis_index("dp"), lax.axis_index("tensor")
        self.sizes = sizes
        self.at = {"z": dp // sizes["y"], "y": dp % sizes["y"], "x": tensor // 2, "c": tensor % 2}

    def moved(self, axis, delta):
        size = self.sizes[axis]
        if size == 2:
            return 1 - self.at[axis]
        return lax.rem(self.at[axis] + (delta % size), size)

    def device(self, **moves):
        at = dict(self.at)
        for axis, delta in moves.items():
            at[axis] = self.moved(axis, delta)
        return (at["z"] * self.sizes["y"] + at["y"], at["x"] * 2 + at["c"])

    def peers(self):
        return self.group() + self.across()

    def group(self):
        return [self.device(x=1), self.device(c=1), self.device(x=1, c=1)]

    def across(self):
        out = [self.device(y=1)]
        for delta in range(1, self.sizes["z"]):
            out += [self.device(z=delta), self.device(z=delta, y=1)]
        return out

    def meet(self):
        barrier = pltpu.get_barrier_semaphore()
        peers = self.peers()
        for peer in peers:
            pl.semaphore_signal(barrier, inc=1, device_id=peer, device_id_type=MESH)
        return lambda: pl.semaphore_wait(barrier, len(peers))


def remote(src, dst, send, recv, device):
    return pltpu.make_async_remote_copy(
        src_ref=src, dst_ref=dst, send_sem=send, recv_sem=recv, device_id=device, device_id_type=MESH
    )


def steps_of(sizes, order):
    out = []
    for axis in order:
        out += ["z1", "z2"] if axis == "z" and sizes["z"] == 4 else [axis]
    return out


def slots_of(sizes, order):
    return sum(2 if step in ("z1", "z2") else sizes[step] - 1 for step in steps_of(sizes, order))


class Gather:
    def __init__(self, place, view, order, rows, send, recv, base):
        self.place, self.view, self.order = place, view, order
        self.send, self.recv, self.base = send, recv, base
        self.low, self.high = pl.ds(0, rows // 2), pl.ds(rows // 2, rows // 2)
        self.steps = steps_of(place.sizes, order)

    def part(self, step, **changed):
        where = dict(self.place.at)
        where["r"] = slice(None)
        for axis in self.order[: self.order.index(self.steps[step][0])]:
            where[axis] = slice(None)
        where.update(changed)
        return self.view(where)

    def copies(self, step):
        name, moved = self.steps[step], self.place.moved
        if name == "z1":
            return [(self.part(step), self.part(step, z=moved("z", -d)), {"z": d}) for d in (1, -1)]
        if name == "z2":
            out = []
            for d, rows in ((1, self.low), (-1, self.high)):
                far = self.part(step, z=moved("z", 2), r=rows)
                out.append((self.part(step, z=moved("z", -d), r=rows), far, {"z": d}))
            return out
        size = self.place.sizes[name]
        return [
            (self.part(step), self.part(step, **{name: moved(name, -d)}), {name: d}) for d in range(1, size)
        ]

    def made(self, step, came):
        slot = self.base
        for index in range(step):
            slot += len(self.copies(index))
        for source, landed, moves in self.copies(step):
            ref = landed if came else source
            yield remote(ref, ref, self.send.at[slot], self.recv.at[slot], self.place.device(**moves))
            slot += 1

    def start(self, step):
        for copy in self.made(step, False):
            copy.start()

    def arrive(self, step):
        for copy in self.made(step, True):
            copy.wait_recv()

    def next(self, step):
        if 0 < step <= len(self.steps):
            self.arrive(step - 1)
        if step < len(self.steps):
            self.start(step)

    def finish(self):
        for step in range(len(self.steps)):
            for copy in self.made(step, False):
                copy.wait_send()


def lanes(shape, limit):
    return lax.broadcasted_iota(jnp.int32, shape, 1) < limit


def token_rows(ref, seq, rows):
    return [ref[pl.ds(2 * j + seq, rows, stride=8), :] for j in range(4)]


def row_mean(parts):
    total = parts[0]
    for part in parts[1:]:
        total = total + part
    return jnp.sum(total, -1, keepdims=True) * (1.0 / (128 * len(parts)))


def normalize(parts):
    mean = row_mean(parts)
    center = [part - mean for part in parts]
    spread = row_mean([part * part for part in center])
    scale = lax.rsqrt(spread + 1e-05)
    return center, scale


def rope(value, cos, sin_a, sin_b):
    return value * cos + pltpu.roll(value, 96, 1) * sin_a + pltpu.roll(value, 32, 1) * sin_b


def rope_back(grad, cos, sin_a, sin_b):
    return grad * cos - pltpu.roll(grad, 96, 1) * sin_a - pltpu.roll(grad, 32, 1) * sin_b


def rope_tables(rows):
    half = HD // 2
    rates = np.exp(np.arange(half, dtype=np.float32) * np.float32(-2.0 * math.log(10000.0) / HD))
    angles = np.arange(rows, dtype=np.float32)[:, None] * rates.astype(np.float32)[None, :]
    cos, sin, zero = np.cos(angles), np.sin(angles), np.zeros_like(angles)
    tables = [[cos] * 4, [-sin, zero] * 2, [zero, sin] * 2]
    return jnp.asarray(np.stack([np.concatenate(table, -1) for table in tables]).astype(np.float32))


class Scatter:
    def __init__(self, place, view, work, order, dims, rows, lead, landing, final, send, recv, base):
        self.place, self.view, self.work, self.order, self.dims = place, view, work, order, dims
        self.lead, self.landing, self.final = lead, landing, final
        self.send, self.recv, self.base = send, recv, base
        self.low, self.high = pl.ds(0, rows // 2), pl.ds(rows // 2, rows // 2)
        self.steps = steps_of(place.sizes, order)

    def done(self, step):
        return self.order[: self.order.index(self.steps[step][0])]

    def part(self, step, kept=False, **changed):
        where = dict(self.place.at)
        where["r"] = slice(None)
        for axis in self.order:
            if axis not in self.done(step):
                where[axis] = slice(None)
        where.update(changed)
        return (self.work if kept or step > 0 else self.view)(where)

    def sends(self, step):
        name, moved = self.steps[step], self.place.moved
        if name == "z1":
            return [({"z": moved("z", 2), "r": rows}, {"z": d}) for d, rows in ((1, self.low), (-1, self.high))]
        if name == "z2":
            return [({"z": moved("z", d)}, {"z": d}) for d in (1, -1)]
        return [({name: moved(name, d)}, {name: d}) for d in range(1, self.place.sizes[name])]

    def sums(self, step):
        name, moved = self.steps[step], self.place.moved
        if name == "z1":
            return [({"z": moved("z", 1), "r": self.low}, [0]), ({"z": moved("z", -1), "r": self.high}, [1])]
        return [({name[0]: self.place.at[name[0]]}, list(range(len(self.sends(step)))))]

    def made(self, step):
        slot = self.base
        for index in range(step):
            slot += len(self.sends(index))
        for index, (where, moves) in enumerate(self.sends(step)):
            yield remote(
                self.part(step, **where),
                self.landing[step].at[index],
                self.send.at[slot + index],
                self.recv.at[slot + index],
                self.place.device(**moves),
            )

    def start(self, step):
        for copy in self.made(step):
            copy.start()

    def arrive(self, step):
        for copy in self.made(step):
            copy.wait_recv()
        axis = self.steps[step][0]
        rest = [a for a in self.dims if a in self.order and a not in self.done(step) and a != axis]
        sizes = [self.place.sizes[a] for a in rest]
        landing = self.landing[step]
        last = step == len(self.steps) - 1
        for where, pieces in self.sums(step):

            def add(index, carry, where=where, pieces=pieces):
                chosen = {}
                for a, size in zip(reversed(rest), reversed(sizes)):
                    chosen[a] = lax.rem(index, size)
                    index = index // size
                total = self.part(step, **chosen, **where)[...].astype(F32)
                for piece in pieces:
                    place = (piece,) + (slice(None),) * self.lead + tuple(chosen[a] for a in rest)
                    total = total + landing[place].astype(F32)
                if last:
                    self.final[...] = total
                else:
                    self.part(step, kept=True, **chosen, **where)[...] = total.astype(BF16)
                return carry

            count = math.prod(sizes)
            if count == 1:
                add(0, 0)
            else:
                lax.fori_loop(0, count, add, 0)

    def next(self, step):
        if 0 < step <= len(self.steps):
            self.arrive(step - 1)
        if step < len(self.steps):
            self.start(step)

    def finish(self):
        for step in range(len(self.steps)):
            for copy in self.made(step):
                copy.wait_send()


def landing_shapes(sizes, order, dims, rows, width, lead=(), lane_x=False):
    left = list(order)
    shapes = []
    for step in steps_of(sizes, order):
        axis = step[0]
        if step != "z2" and axis in left:
            left.remove(axis)
        count = 2 if step in ("z1", "z2") else sizes[axis] - 1
        high = rows // 2 if step == "z1" else rows
        wide = width * 2 if lane_x and "x" in left else width
        shapes.append((count,) + lead + tuple(sizes[a] for a in dims if a in left) + (high, wide))
    return shapes


def gelu_parts(value):
    cdf = 0.5 + 0.5 * lax.erf(value * (2.0**-0.5))
    density = jnp.exp(-0.5 * value * value) * ((2.0 * math.pi) ** -0.5)
    return value * cdf, cdf + value * density


GATHERS = (
    ("q", "zyx"),
    ("k", "xzy"),
    ("v", "xyz"),
    ("n", "zy"),
    ("out", "zyxc"),
    ("u0", "xzyc"),
    ("u1", "yzxc"),
    ("d0", "xyzc"),
    ("d1", "xyzc"),
)
SCATTERS = (
    ("d0", "czyx", "xczy", 256, False),
    ("d1", "cxzy", "xczy", 256, False),
    ("u0", "czxy", "xczy", 256, False),
    ("u1", "czyx", "xczy", 256, False),
    ("out", "cyzx", "czy", 128, True),
    ("q", "zyx", "zy", 128, True),
    ("k", "zxy", "zy", 128, True),
    ("v", "yxz", "zy", 128, True),
)
GATHER_AT = dict(
    f0=dict(q=(0,), k=(0,), v=(0,), n=(0,), out=(0,), u0=(0,), u1=(0,), d1=(0,)),
    f1=dict(q=(1,), k=(1,), v=(1,), u1=(1,)),
    f2=dict(q=(2,), k=(2,), v=(2,), out=(1,), u0=(1,), d1=(1,)),
    f3=dict(q=(3,), k=(3,), n=(1,), out=(2,), d0=(0,)),
    f4=dict(u1=(2,)),
    f5=dict(v=(3,), u0=(2,)),
    f6=dict(n=(2,), u1=(3,)),
    f7=dict(q=(4,), k=(4,), v=(4,)),
    pr1=dict(d1=(2,)),
    a=dict(d0=(1,)),
    m0=dict(out=(3,)),
    b0=dict(n=(3,), u0=(3,)),
    m2=dict(d0=(2,)),
    b2=dict(u1=(4,), d1=(3,)),
    b3=dict(out=(4,), u0=(4,), d0=(3,)),
    e0=dict(out=(5,), u1=(5,), d0=(4,), d1=(4,)),
    e1=dict(u0=(5,)),
    e2=dict(d0=(5,), d1=(5,)),
)
SCATTER_AT = dict(
    g0=dict(d0=(0,), d1=(0,)),
    g1=dict(u0=(0,), u1=(0,)),
    g2=dict(d0=(1,), u0=(1,)),
    g3=dict(d1=(1,), u1=(1,), out=(0,)),
    g4=dict(d0=(2,), u0=(2,), u1=(2,), out=(1,)),
    q0=dict(q=(0,)),
    q1=dict(u0=(3,), k=(0,)),
    q2=dict(v=(0,)),
    q3=dict(d0=(3,), d1=(2,), u1=(3,), out=(2,), q=(1,)),
    z0=dict(k=(1,), v=(1,)),
    z1=dict(d1=(3,), u0=(4,), u1=(4,), out=(3,), q=(2,), k=(2,), v=(2,)),
    z2=dict(d0=(4,), d1=(4,), out=(4,), q=(3,), k=(3,), v=(3,)),
    z3=dict(d0=(5,), d1=(5,), u0=(5,), u1=(5,), out=(5,), q=(4,), k=(4,), v=(4,)),
)
HEADS = ("q", "k", "v")


def x_lane(index):
    return index if isinstance(index, slice) else pl.ds(pl.multiple_of(index * 128, 128), 128)


class Refs:
    pass


class Layer:
    def __init__(self, sizes, rows, tokens_total, refs):
        self.r = refs
        self.sizes, self.rows, self.own, self.tokens_total = sizes, rows, rows // 4, tokens_total
        self.place = Place(sizes)
        at = self.place.at
        self.x, self.c, self.z, self.y = at["x"], at["c"], at["z"], at["y"]
        self.t = self.x * 2 + self.c
        self.shard = 512 // (sizes["z"] * sizes["y"])
        self.half = lanes((self.own, 128), HD)
        self.zero = jnp.zeros((self.own, 128), BF16)
        self.gathers = self.make_gathers()
        self.scatters = self.make_scatters()
        self.sent = []

    def make_gathers(self):
        r = self.r

        def qkv_view(i):
            return lambda w: r.qkv_all.at[i, w["z"], w["y"], w["r"], x_lane(w["x"])]

        def ff_view(start):
            return lambda w: r.ff_all.at[w["x"], w["c"], w["z"], w["y"], w["r"], pl.ds(start, 256)]

        views = {
            "q": qkv_view(0),
            "k": qkv_view(1),
            "v": qkv_view(2),
            "n": lambda w: r.counts.at[w["z"], w["y"], w["r"]],
            "out": lambda w: r.out_all.at[w["c"], w["z"], w["y"], w["r"], x_lane(w["x"])],
            "u0": ff_view(0),
            "u1": ff_view(256),
            "d0": ff_view(512),
            "d1": ff_view(768),
        }
        plans, base = {}, 0
        for name, order in GATHERS:
            rows = 16 if name == "n" else self.shard
            plans[name] = Gather(self.place, views[name], order, rows, r.send_w, r.recv_w, base)
            base += slots_of(self.sizes, order)
        return plans

    def make_scatters(self):
        r = self.r

        def ff_view(start):
            return lambda w: r.grad_ff.at[w["x"], w["c"], w["z"], w["y"], w["r"], pl.ds(start, 256)]

        def ff_kept(start):
            return lambda w: r.ff_work.at[w["x"], w["z"], w["y"], w["r"], pl.ds(start, 256)]

        def qkv_view(i):
            return lambda w: r.grad_qkv.at[i, w["z"], w["y"], w["r"], x_lane(w["x"])]

        views = {
            "u0": (ff_view(0), ff_kept(0), r.up_final.at[:, pl.ds(0, 256)]),
            "u1": (ff_view(256), ff_kept(256), r.up_final.at[:, pl.ds(256, 256)]),
            "d0": (ff_view(512), ff_kept(512), r.down_final.at[:, pl.ds(0, 256)]),
            "d1": (ff_view(768), ff_kept(768), r.down_final.at[:, pl.ds(256, 256)]),
            "out": (
                lambda w: r.grad_out.at[w["c"], w["z"], w["y"], w["r"], x_lane(w["x"])],
                lambda w: r.out_work.at[w["z"], w["y"], w["r"], x_lane(w["x"])],
                r.out_final,
            ),
        }
        for i, name in enumerate("qkv"):
            views[name] = (qkv_view(i), qkv_view(i), r.qkv_final.at[i])
        plans, base, used = {}, 0, 0
        for name, order, dims, width, lane_x in SCATTERS:
            view, kept, final = views[name]
            count = len(steps_of(self.sizes, order))
            landing = r.landing[used : used + count]
            plans[name] = Scatter(
                self.place, view, kept, order, dims, self.shard, 0, landing, final, r.send_g, r.recv_g, base
            )
            used += count
            base += slots_of(self.sizes, order)
        return plans

    def point(self, label):
        for plans, places in ((self.gathers, GATHER_AT), (self.scatters, SCATTER_AT)):
            for name, steps in places.get(label, {}).items():
                for step in steps:
                    plans[name].next(step)

    def within(self, index, label):
        if label in GATHER_AT or label in SCATTER_AT:

            @pl.when(index)
            def _():
                self.point(label)

    def local(self, index, src, dst):
        copy = pltpu.make_async_copy(src, dst, self.r.local_sem.at[index])
        copy.start()
        return copy

    def row_block(self, index):
        return pl.ds(pl.multiple_of(index * self.own, self.own), self.own)

    def run(self):
        self.front()
        self.attention()
        self.feed_forward()
        self.attention_back()
        self.end()

    def front(self):
        r, place, x, c, own = self.r, self.place, self.x, self.c, self.own
        met = place.meet()
        copies = [
            self.local(0, r.qkv_shard, r.qkv_all.at[:, self.z, self.y, :, x_lane(x)]),
            self.local(1, r.out_shard, r.out_all.at[c, self.z, self.y, :, x_lane(x)]),
            self.local(2, r.up_shard, r.ff_all.at[x, c, self.z, self.y, :, pl.ds(0, 512)]),
            self.local(3, r.down_shard, r.ff_all.at[x, c, self.z, self.y, :, pl.ds(512, 512)]),
        ]
        load_x = self.local(4, r.x_hbm, r.x_ref)
        load_tables = self.local(5, r.tables_hbm, r.tables)
        self.loads = [self.local(6, r.teacher_hbm, r.teacher), self.local(7, r.cotangent_hbm, r.cotangent)]
        total = r.lengths[0] + r.lengths[1]
        r.counts[self.z, self.y] = jnp.full((16, 128), total.astype(F32))
        for copy in copies:
            copy.wait()
        met()
        self.point("f0")
        load_x.wait()
        for s in range(2):
            center, scale = normalize(token_rows(r.x_ref, s, own))
            for j in range(4):
                lane = pl.ds(128 * j, 128)
                value = center[j] * scale * r.gain_1[:, lane] + r.shift_1[:, lane]
                r.own_normed[s, :, lane] = value.astype(BF16)
        mine = self.row_block(self.t)

        def tokens(index, ref, moves):
            return remote(ref, ref, r.send_n.at[index], r.recv_n.at[index], place.device(**moves))

        sent = [
            remote(r.own_normed.at[1 - x], r.normed_all.at[mine], r.send_n.at[0], r.recv_n.at[0], place.device(x=1)),
            remote(r.own_normed.at[x], r.normed_all.at[mine], r.send_n.at[1], r.recv_n.at[1], place.device(c=1)),
        ]
        for copy in sent:
            copy.start()
        keep = self.local(0, r.own_normed.at[x], r.normed_all.at[mine])
        for label in ("f1", "f2", "f3"):
            self.point(label)
        far = r.normed_all.at[self.row_block((1 - x) * 2 + c)]
        tokens(0, far, {"x": 1}).wait_recv()
        sent.append(tokens(2, far, {"c": 1}))
        sent[-1].start()
        self.point("f4")
        self.point("f5")
        keep.wait()
        tokens(1, r.normed_all.at[self.row_block(x * 2 + 1 - c)], {"c": 1}).wait_recv()
        self.point("f6")
        tokens(2, r.normed_all.at[self.row_block((1 - x) * 2 + 1 - c)], {"c": 1}).wait_recv()
        self.point("f7")
        load_tables.wait()
        self.sent += sent

        w_qkv = [r.qkv_all[i].reshape(-1, 256) for i in range(3)]

        def project(index, carry):
            here = pl.ds(pl.multiple_of(index * own, own), own)
            normed = r.normed_all[here, :]
            cos, sin_a, sin_b = (r.tables[i, here, :] for i in range(3))
            for i, ref in ((0, r.q_all), (1, r.k_all), (2, r.v_all)):
                value = dot(normed, w_qkv[i])
                for pair in range(2):
                    lane = pl.ds(128 * pair, 128)
                    part = value[:, 128 * pair : 128 * pair + 128]
                    if i < 2:
                        part = rope(part, cos, sin_a, sin_b)
                    if i == 0:
                        part = part.astype(BF16) * jnp.asarray(HD**-0.5, BF16)
                    ref[here, lane] = part.astype(BF16)
            self.within(index == 1, "pr1")
            return carry

        lax.fori_loop(0, 4, project, 0)
        self.point("a")

    def hand(self, qb, act):
        r, t = self.r, self.t
        source, target = r.own_attended.at[pl.ds(qb * self.own, self.own)], r.attended.at[self.c, self.x]
        device = (lax.axis_index("dp"), jnp.asarray(qb, jnp.int32))

        @pl.when(t != qb)
        def _():
            copy = remote(source, target, r.send_a.at[qb], r.recv_a.at[t], device)
            copy.start() if act == "start" else copy.wait_send()

        if act == "start":

            @pl.when(t == qb)
            def _():
                pltpu.make_async_copy(source, target, r.recv_a.at[t]).start()

    def attention(self):
        r, own, half, zero = self.r, self.own, self.half, self.zero
        length = r.lengths[self.x]
        for qb in range(4):
            here = pl.ds(qb * own, own)
            keys = (qb + 1) * own
            key_pos = lax.broadcasted_iota(jnp.int32, (own, keys), 1)
            query_pos = lax.broadcasted_iota(jnp.int32, (own, keys), 0) + qb * own
            allowed = key_pos <= query_pos
            if qb > 1:
                allowed = allowed & (key_pos < length)

            def attend(pair, carry, qb=qb, here=here, keys=keys, allowed=allowed):
                lane = pl.ds(pl.multiple_of(pair * 128, 128), 128)
                queries = r.q_all[here, lane]
                k_part = r.k_all[pl.ds(0, keys), lane]
                v_part = r.v_all[pl.ds(0, keys), lane]
                mixed = []
                for head in range(2):
                    masked = jnp.where(half, queries, zero) if head == 0 else jnp.where(half, zero, queries)
                    scores = jnp.where(allowed, dot(masked, k_part, NT), -1e30)
                    highest = jnp.max(scores, -1, keepdims=True)
                    expd = jnp.exp(scores - highest)
                    denom = jnp.sum(expd, -1, keepdims=True)
                    probs = (expd * (1.0 / denom)).astype(BF16)
                    mixed.append(dot(probs, v_part))
                    wide = jnp.broadcast_to(highest + jnp.log(denom), (own, 128))
                    r.lse[pair * 2 + head, :, here] = jnp.transpose(wide)[:8]
                r.own_attended[here, lane] = jnp.where(half, mixed[0], mixed[1]).astype(BF16)
                self.within(pair == 0, "m%d" % qb)
                return carry

            lax.fori_loop(0, 2, attend, 0)
            self.hand(qb, "start")
            self.point("b%d" % qb)
        for pair in range(2):
            r.k_t[pair] = jnp.transpose(r.k_all[:, pl.ds(128 * pair, 128)])
        for k in range(2):
            for s in range(2):
                came = r.attended.at[k, s]
                remote(came, came, r.send_a.at[0], r.recv_a.at[s * 2 + k], self.place.device(x=1)).wait_recv()

    def feed_forward(self):
        r, own = self.r, self.own
        self.point("e0")
        count = jnp.sum(r.counts[...], axis=(0, 1))[0:1]
        factor = self.tokens_total / count
        weights = [r.out_all[k].reshape(512, 256) for k in range(2)]
        valid = []
        for s in range(2):
            rows = pl.ds(s * own, own)
            attn = dot(r.attended[0, s], weights[0], NT) + dot(r.attended[1, s], weights[1], NT)
            parts = token_rows(r.x_ref, s, own)
            for j in range(4):
                r.middle[rows, pl.ds(128 * j, 128)] = parts[j] + attn[:, 128 * j : 128 * j + 128]
            position = self.t * own + lax.broadcasted_iota(jnp.int32, (own, 128), 0)
            valid.append((position < r.lengths[s]).astype(F32))
        value = r.middle[...]
        mean = jnp.mean(value, -1, keepdims=True)
        center = value - mean
        scale = lax.rsqrt(jnp.mean(center * center, -1, keepdims=True) + 1e-05)
        normed = (center * scale * r.gain_2[...] + r.shift_2[...]).astype(BF16)
        normed_t = jnp.transpose(normed)

        def weight(t, start):
            return r.ff_all[t // 2, t % 2, :, :, :, pl.ds(start, 512)].reshape(512, 512)

        self.point("e1")

        def up(t, carry):
            act, slope = gelu_parts(dot(normed, weight(t, 0)))
            r.slope[t] = slope
            r.hidden[t] = act.astype(BF16)
            return carry

        lax.fori_loop(0, 4, up, 0)
        self.point("e2")
        r.total_sum[...] = jnp.zeros_like(r.total_sum)

        def down(t, carry):
            r.total_sum[...] += dot(r.hidden[t], weight(t, 512), NT)
            return carry

        lax.fori_loop(0, 4, down, 0)
        self.point("e3")
        for copy in self.loads:
            copy.wait()
        square = jnp.zeros((own, 128), F32)
        for s in range(2):
            rows = pl.ds(s * own, own)
            want = token_rows(r.teacher, s, own)
            pull = token_rows(r.cotangent, s, own)
            for j in range(4):
                lane = pl.ds(128 * j, 128)
                out = r.middle[rows, lane] + r.total_sum[rows, lane]
                r.output[pl.ds(2 * j + s, own, stride=8), :] = out
                differ = out - want[j]
                square = square + valid[s] * differ * differ
                r.seed[rows, lane] = factor * valid[s] * (pull[j] + differ)
        self.store = self.local(6, r.output, r.output_hbm)
        grad_f = r.seed[...].astype(BF16)
        grad_f_t = jnp.transpose(grad_f)
        r.total_sum[...] = jnp.zeros_like(r.total_sum)

        def put(t, start, value):
            value = value.astype(BF16).reshape(self.sizes["z"], self.sizes["y"], self.shard, 512)
            r.grad_ff[t // 2, t % 2, :, :, :, pl.ds(start, 512)] = value

        def back_down(t, carry):
            put(t, 512, dot(grad_f_t, r.hidden[t]))
            return carry

        lax.fori_loop(0, 4, back_down, 0)
        self.point("g0")

        def back_up(t, carry):
            grad_before = (r.slope[t] * dot(grad_f, weight(t, 512))).astype(BF16)
            put(t, 0, dot(normed_t, grad_before))
            r.total_sum[...] += dot(grad_before, weight(t, 0), NT)
            return carry

        lax.fori_loop(0, 4, back_up, 0)
        self.point("g1")
        grad_normed = r.total_sum[...]
        unit = (r.middle[...] - mean) * scale
        r.stat_send[0] = jnp.zeros_like(r.stat_send[0])
        r.stat_send[0, 0:1, 0:128] = jnp.sum(square, 0, keepdims=True)
        r.stat_send[0, 1:2] = jnp.sum(grad_normed * unit, 0, keepdims=True)
        r.stat_send[0, 2:3] = jnp.sum(grad_normed, 0, keepdims=True)
        scaled = grad_normed * r.gain_2[...]
        inner = jnp.mean(scaled * unit, -1, keepdims=True)
        grad = r.seed[...] + scale * (scaled - jnp.mean(scaled, -1, keepdims=True) - unit * inner)
        r.grad_middle[...] = grad
        branch = grad.astype(BF16)
        for k in range(2):
            grads = dot(branch, weights[k]).astype(BF16)
            for s in range(2):
                r.grad_attended[k, s] = grads[s * own : s * own + own]
        self.send_attended_back()
        self.point("g2")
        branch_t = jnp.transpose(branch)
        for k in range(2):
            value = dot(branch_t[:, :own], r.attended[k, 0]) + dot(branch_t[:, own:], r.attended[k, 1])
            r.grad_out[k] = value.astype(BF16).reshape(self.sizes["z"], self.sizes["y"], self.shard, 256)
        self.point("g3")

    def send_attended_back(self):
        r, at = self.r, self.place.at
        mine = r.g_all.at[self.row_block(self.t)]
        for index, moves in enumerate(({"x": 1}, {"x": 1, "c": 1}, {"c": 1})):
            to = dict(at)
            for axis in moves:
                to[axis] = 1 - at[axis]
            source = r.grad_attended.at[to["c"], to["x"]]
            copy = remote(source, mine, r.send_b.at[index], r.recv_b.at[self.t], self.place.device(**moves))
            copy.start()
            self.sent.append(copy)
        pltpu.make_async_copy(r.grad_attended.at[self.c, self.x], mine, r.recv_b.at[self.t]).start()

    def to_core(self, qb, act):
        r, i = self.r, qb // 2

        @pl.when(self.c != qb % 2)
        def _():
            source = r.grad_n.at[pl.ds(qb * self.own, self.own)]
            copy = remote(source, r.from_core.at[i], r.send_n.at[3 + i], r.recv_n.at[3 + i], self.place.device(c=1))
            copy.start() if act == "start" else copy.wait_send()

    def core_arrived(self, index):
        r = self.r
        slot = r.from_core.at[index]
        remote(slot, slot, r.send_n.at[3], r.recv_n.at[3 + index], self.place.device(c=1)).wait_recv()

    def cross(self):
        r = self.r
        return remote(r.to_x, r.from_x, r.send_n.at[5], r.recv_n.at[5], self.place.device(x=1))

    def to_chip(self, qb):
        r = self.r

        @pl.when((self.c == qb % 2) & (self.x != qb // 2))
        def _():
            self.core_arrived(qb // 2)
            r.to_x[...] = (r.grad_n[pl.ds(qb * self.own, self.own), :] + r.from_core[qb // 2]).astype(BF16)
            self.cross().start()

    def attention_back(self):
        r, own, half, zero = self.r, self.own, self.half, self.zero
        normed_t = jnp.transpose(r.normed_all[...])
        length = r.lengths[self.x]
        upper = lax.broadcasted_iota(jnp.int32, (128, own), 0) < HD
        w_qkv = [r.qkv_all[i].reshape(512, 256) for i in range(3)]
        self.point("g4")
        for qb in range(3, -1, -1):
            here = pl.ds(qb * own, own)
            keys = (qb + 1) * own
            seen = pl.ds(0, keys)
            key_pos = lax.broadcasted_iota(jnp.int32, (keys, own), 0)
            query_pos = lax.broadcasted_iota(jnp.int32, (keys, own), 1) + qb * own
            allowed = key_pos <= query_pos
            if qb > 1:
                allowed = allowed & (key_pos < length)
            came = r.g_all.at[here]
            remote(came, came, r.send_b.at[0], r.recv_b.at[qb], self.place.device(x=1)).wait_recv()

            def attend(pair, carry, qb=qb, here=here, seen=seen, allowed=allowed):
                lane = pl.ds(pl.multiple_of(pair * 128, 128), 128)
                queries = r.q_all[here, lane]
                grads = r.g_all[here, lane]
                k_part = r.k_all[seen, lane]
                v_part = r.v_all[seen, lane]
                dq = []
                for head in range(2):
                    if head == 0:
                        q_m, g_m = jnp.where(half, queries, zero), jnp.where(half, grads, zero)
                    else:
                        q_m, g_m = jnp.where(half, zero, queries), jnp.where(half, zero, grads)
                    scores = dot(k_part, q_m, NT)
                    probs = jnp.where(allowed, jnp.exp(scores - r.lse[pair * 2 + head, 0:1, here]), 0.0)
                    grad_probs = dot(v_part, g_m, NT)
                    inner = jnp.sum(probs * grad_probs, 0, keepdims=True)
                    grad_raw = (probs * (grad_probs - inner)).astype(BF16)
                    add_k = dot(grad_raw, q_m)
                    add_v = dot(probs.astype(BF16), g_m)
                    if qb == 3 and head == 0:
                        r.grad_k[seen, lane] = add_k
                        r.grad_v[seen, lane] = add_v
                    else:
                        r.grad_k[seen, lane] += add_k
                        r.grad_v[seen, lane] += add_v
                    dq.append(dot(r.k_t[pair, :, seen], grad_raw))
                r.grad_q[here, lane] = jnp.transpose(jnp.where(upper, dq[0], dq[1])) * HD**-0.5
                self.within(pair == 0, "n%d" % qb)
                return carry

            lax.fori_loop(0, 2, attend, 0)

            cos, sin_a, sin_b = (r.tables[i, here, :] for i in range(3))
            total = jnp.zeros((own, 512), F32)
            for i, ref in ((0, r.grad_q), (1, r.grad_k), (2, r.grad_v)):
                for pair in range(2):
                    lane = pl.ds(128 * pair, 128)
                    part = ref[here, lane]
                    if i < 2:
                        part = rope_back(part, cos, sin_a, sin_b)
                    r.grad_proj[i, here, lane] = part.astype(BF16)
                total = total + dot(r.grad_proj[i, here, :], w_qkv[i], NT)
            r.grad_n[here, :] = total
            self.to_core(qb, "start")
            if qb < 3:
                self.to_chip(qb + 1)
            self.point("t%d" % qb)
        for i, name in enumerate(HEADS):
            value = dot(normed_t, r.grad_proj[i]).astype(BF16)
            r.grad_qkv[i] = value.reshape(self.sizes["z"], self.sizes["y"], self.shard, 256)
            if i == 1:
                self.to_chip(0)
            self.point("q%d" % i)

    def end(self):
        r, own, x = self.r, self.own, self.x
        self.point("q3")
        self.core_arrived(x)
        self.cross().wait_recv()
        self.point("z0")
        grad_gain = [jnp.zeros((1, 128), F32)] * 4
        grad_shift = [jnp.zeros((1, 128), F32)] * 4
        for s in range(2):
            center, scale = normalize(token_rows(r.x_ref, s, own))
            near = r.grad_n[self.row_block(self.t), :] + r.from_core[x]
            chosen = jnp.where(x == s, near, r.from_x[...].astype(F32))
            grads = [chosen[:, 128 * j : 128 * j + 128] for j in range(4)]
            units = [part * scale for part in center]
            scaled = [grads[j] * r.gain_1[:, pl.ds(128 * j, 128)] for j in range(4)]
            mean = row_mean(scaled)
            inner = row_mean([scaled[j] * units[j] for j in range(4)])
            for j in range(4):
                part = r.grad_middle[pl.ds(s * own, own), pl.ds(128 * j, 128)]
                grad = part + scale * (scaled[j] - mean - units[j] * inner)
                r.grad_inputs[pl.ds(2 * j + s, own, stride=8), :] = grad
                grad_gain[j] = grad_gain[j] + jnp.sum(grads[j] * units[j], 0, keepdims=True)
                grad_shift[j] = grad_shift[j] + jnp.sum(grads[j], 0, keepdims=True)
        for j in range(4):
            r.stat_send[0, 3:4, 128 * j : 128 * j + 128] = grad_gain[j]
            r.stat_send[0, 4:5, 128 * j : 128 * j + 128] = grad_shift[j]
        slot = 0
        for phase, peers in enumerate((self.place.group(), self.place.across())):
            came = []
            for peer in peers:
                came.append(
                    remote(r.stat_send.at[phase], r.stat_land.at[slot], r.send_s.at[slot], r.recv_s.at[slot], peer)
                )
                came[-1].start()
                slot += 1
            self.point("z%d" % (phase + 1))
            total = r.stat_send[phase]
            for index, copy in enumerate(came):
                copy.wait_recv()
                total = total + r.stat_land[slot - len(came) + index]
            if phase == 0:
                r.stat_send[1] = total
            else:
                r.stats_final[...] = total
            self.sent += came
        self.point("z3")
        for plan in list(self.gathers.values()) + list(self.scatters.values()):
            plan.finish()
        for copy in self.sent + [self.cross()]:
            copy.wait_send()
        for qb in range(4):
            self.hand(qb, "finish")
            self.to_core(qb, "finish")
        self.store.wait()


def whole(sizes, rows, tokens_total, operands):
    zs, ys = sizes["z"], sizes["y"]
    shard = 512 // (zs * ys)
    own = rows // 4
    wide = own * 8
    inputs = dict(
        lengths=0, gain_1=0, shift_1=0, gain_2=0, shift_2=0, x_hbm=0,
        teacher_hbm=0, cotangent_hbm=0, tables_hbm=0, qkv_shard=0, out_shard=0, up_shard=0, down_shard=0,
    )
    outputs = dict(
        output_hbm=(wide, 128),
        grad_inputs=(wide, 128),
        up_final=(shard, 512),
        down_final=(shard, 512),
        out_final=(shard, 128),
        qkv_final=(3, shard, 128),
        stats_final=(8, 512),
        counts=(zs, ys, 16, 128),
    )
    scratch = dict(
        x_ref=((wide, 128), F32),
        teacher=((wide, 128), F32),
        cotangent=((wide, 128), F32),
        output=((wide, 128), F32),
        tables=((3, rows, 128), F32),
        ff_all=((2, 2, zs, ys, shard, 1024), BF16),
        out_all=((2, zs, ys, shard, 256), BF16),
        qkv_all=((3, zs, ys, shard, 256), BF16),
        own_normed=((2, own, 512), BF16),
        normed_all=((rows, 512), BF16),
        q_all=((rows, 256), BF16),
        k_all=((rows, 256), BF16),
        v_all=((rows, 256), BF16),
        k_t=((2, 128, rows), BF16),
        lse=((4, 8, rows), F32),
        own_attended=((rows, 256), BF16),
        attended=((2, 2, own, 256), BF16),
        middle=((2 * own, 512), F32),
        seed=((2 * own, 512), F32),
        slope=((4, 2 * own, 512), F32),
        hidden=((4, 2 * own, 512), BF16),
        total_sum=((2 * own, 512), F32),
        grad_middle=((2 * own, 512), F32),
        grad_attended=((2, 2, own, 256), BF16),
        grad_ff=((2, 2, zs, ys, shard, 1024), BF16),
        grad_out=((2, zs, ys, shard, 256), BF16),
        g_all=((rows, 256), BF16),
        grad_q=((rows, 256), F32),
        grad_k=((rows, 256), F32),
        grad_v=((rows, 256), F32),
        grad_proj=((3, rows, 256), BF16),
        grad_qkv=((3, zs, ys, shard, 256), BF16),
        grad_n=((rows, 512), F32),
        ff_work=((2, zs, ys, shard, 1024), BF16),
        out_work=((zs, ys, shard, 256), BF16),
        from_core=((2, own, 512), F32),
        to_x=((own, 512), BF16),
        from_x=((own, 512), BF16),
        stat_send=((2, 8, 512), F32),
        stat_land=((zs * ys + 2, 8, 512), F32),
    )
    gathered = sum(slots_of(sizes, order) for _, order in GATHERS)
    scattered = sum(slots_of(sizes, item[1]) for item in SCATTERS)
    sems = dict(local_sem=8, send_w=gathered, recv_w=gathered, send_g=scattered, recv_g=scattered)
    sems |= dict(send_n=6, recv_n=6, send_a=4, recv_a=4, send_b=3, recv_b=4)
    sems |= dict(send_s=zs * ys + 2, recv_s=zs * ys + 2)
    lands = []
    for _, order, dims, width, lane_x in SCATTERS:
        lands += landing_shapes(sizes, order, dims, shard, width, lane_x=lane_x)

    def kernel(*refs):
        refs = list(refs)
        out = Refs()
        for name in list(inputs) + list(outputs) + list(scratch) + list(sems):
            setattr(out, name, refs.pop(0))
        out.landing = refs
        Layer(sizes, rows, tokens_total, out).run()

    any_spec = pl.BlockSpec(memory_space=pl.ANY)
    vmem = pl.BlockSpec(memory_space=pltpu.VMEM)
    return pl.pallas_call(
        kernel,
        out_shape=[jax.ShapeDtypeStruct(shape, F32) for shape in outputs.values()],
        in_specs=[pl.BlockSpec(memory_space=pltpu.SMEM)] + [vmem] * 4 + [any_spec] * 8,
        out_specs=[any_spec] + [vmem] * (len(outputs) - 1),
        scratch_shapes=[pltpu.VMEM(*shape) for shape in scratch.values()]
        + [pltpu.SemaphoreType.DMA((count,)) for count in sems.values()]
        + [pltpu.VMEM(shape, BF16) for shape in lands],
        name="whole",
        compiler_params=pltpu.CompilerParams(
            collective_id=0, has_side_effects=True, vmem_limit_bytes=VMEM_LIMIT
        ),
    )(*operands)


def last_kernel(features, counts, output, grad_inputs, up, down, out, qkv, sums, *outs):
    for source, target in zip((output, grad_inputs, up, down, out, qkv), outs[:6]):
        target[...] = source[...]
    for target, row in zip(outs[6:10], (3, 4, 1, 2)):
        target[...] = sums[row : row + 1]
    total = jnp.sum(counts[...], axis=0)[0:1, 0:1]
    outs[10][...] = jnp.sum(sums[0:1, 0:128], -1, keepdims=True) / (total * features)


def last(features, counts, output, grad_inputs, up, down, out, qkv, sums):
    vmem = pl.BlockSpec(memory_space=pltpu.VMEM)
    shapes = [value.shape for value in (output, grad_inputs, up, down, out, qkv)] + [(1, features)] * 4 + [(1, 1)]
    return pl.pallas_call(
        lambda *refs: last_kernel(features, *refs),
        out_shape=[jax.ShapeDtypeStruct(shape, F32) for shape in shapes],
        in_specs=[vmem] * 8,
        out_specs=[vmem] * len(shapes),
        name="last",
        compiler_params=pltpu.CompilerParams(vmem_limit_bytes=VMEM_LIMIT),
    )(counts, output, grad_inputs, up, down, out, qkv, sums)


def solution(mesh):
    dp, tensor = mesh.shape["dp"], mesh.shape["tensor"]
    sizes = {"z": dp // 2, "y": 2, "x": tensor // 2, "c": 2}

    def shards(
        inputs, qkv_weight, out_weight, up_weight, down_weight, gain_one, shift_one, gain_two, shift_two, lengths,
        teacher, cotangent,
    ):
        own, sequences, width = inputs.shape
        rows = own * tensor

        def packed(value):
            view = value.reshape(own, sequences, width // 128, 128).transpose(0, 2, 1, 3)
            return view.reshape(own * sequences * (width // 128), 128)

        def unpacked(value):
            view = value.reshape(own, width // 128, sequences, 128).transpose(0, 2, 1, 3)
            return view.reshape(own, sequences, width)

        operands = (
            lengths, gain_one[None], shift_one[None], gain_two[None], shift_two[None], packed(inputs), packed(teacher),
            packed(cotangent), rope_tables(rows), qkv_weight, out_weight.T, up_weight, down_weight.T,
        )
        *parts, sums, counts = whole(sizes, rows, float(rows * sequences * dp), operands)
        output, grad_inputs, up, down, out, qkv, gain_1, shift_1, gain_2, shift_2, loss = last(
            width, counts.reshape(dp, 16, 128), *parts, sums
        )
        return (
            unpacked(output), loss.reshape(()), unpacked(grad_inputs), qkv, out.T, up, down.T, gain_1.reshape(width),
            shift_1.reshape(width), gain_2.reshape(width), shift_2.reshape(width),
        )

    tokens, rows_dp, cols_dp = P("tensor", "dp", None), P("dp", "tensor"), P("tensor", "dp")
    heads = P(None, "dp", "tensor")
    return jax.shard_map(
        shards,
        mesh=mesh,
        in_specs=(tokens, heads, cols_dp, rows_dp, cols_dp, P(), P(), P(), P(), P("dp"), tokens, tokens),
        out_specs=(tokens, P(), tokens, heads, cols_dp, rows_dp, cols_dp, P(), P(), P(), P()),
        check_vma=False,
    )
```

```python
import math

import jax
import jax.numpy as jnp
import numpy as np
from jax import lax
from jax.experimental import pallas as pl
from jax.experimental.pallas import tpu as pltpu
from jax.sharding import PartitionSpec as P

HD = 64
F32 = jnp.float32
BF16 = jnp.bfloat16
MESH = pl.DeviceIdType.MESH
VMEM_LIMIT = 60 * 1024 * 1024

NN = (((1,), (0,)), ((), ()))
NT = (((1,), (1,)), ((), ()))


def dot(a, b, dims=NN):
    return lax.dot_general(a, b, dims, preferred_element_type=F32)


class Place:
    def __init__(self, sizes):
        dp, tensor = lax.axis_index("dp"), lax.axis_index("tensor")
        self.sizes = sizes
        self.at = {"z": dp // sizes["y"], "y": dp % sizes["y"], "x": tensor // 2, "c": tensor % 2}

    def moved(self, axis, delta):
        size = self.sizes[axis]
        if size == 2:
            return 1 - self.at[axis]
        return lax.rem(self.at[axis] + (delta % size), size)

    def device(self, **moves):
        at = dict(self.at)
        for axis, delta in moves.items():
            at[axis] = self.moved(axis, delta)
        return (at["z"] * self.sizes["y"] + at["y"], at["x"] * 2 + at["c"])

    def peers(self):
        return self.group() + self.across()

    def group(self):
        return [self.device(x=1), self.device(c=1), self.device(x=1, c=1)]

    def across(self):
        out = [self.device(y=1)]
        for delta in range(1, self.sizes["z"]):
            out += [self.device(z=delta), self.device(z=delta, y=1)]
        return out

    def meet(self):
        barrier = pltpu.get_barrier_semaphore()
        peers = self.peers()
        for peer in peers:
            pl.semaphore_signal(barrier, inc=1, device_id=peer, device_id_type=MESH)
        return lambda: pl.semaphore_wait(barrier, len(peers))


def remote(src, dst, send, recv, device):
    return pltpu.make_async_remote_copy(
        src_ref=src, dst_ref=dst, send_sem=send, recv_sem=recv, device_id=device, device_id_type=MESH
    )


def steps_of(sizes, order):
    out = []
    for axis in order:
        if axis in "zZ":
            out += ["z1", "z2"] if axis == "z" and sizes["z"] == 4 else ["Z"]
        else:
            out.append(axis)
    return out


def axis_of(step):
    return step[0].lower()


def slots_of(sizes, order):
    return sum(2 if step in ("z1", "z2") else sizes[axis_of(step)] - 1 for step in steps_of(sizes, order))


class Gather:
    def __init__(self, place, view, order, rows, send, recv, base):
        self.place, self.view, self.order = place, view, order
        self.send, self.recv, self.base = send, recv, base
        self.low, self.high = pl.ds(0, rows // 2), pl.ds(rows // 2, rows // 2)
        self.steps = steps_of(place.sizes, order)
        self.order = order.lower()

    def part(self, step, **changed):
        where = dict(self.place.at)
        where["r"] = slice(None)
        for axis in self.order[: self.order.index(axis_of(self.steps[step]))]:
            where[axis] = slice(None)
        where.update(changed)
        return self.view(where)

    def copies(self, step):
        name, moved = self.steps[step], self.place.moved
        if name == "z1":
            return [(self.part(step), self.part(step, z=moved("z", -d)), {"z": d}) for d in (1, -1)]
        if name == "z2":
            out = []
            for d, rows in ((1, self.low), (-1, self.high)):
                far = self.part(step, z=moved("z", 2), r=rows)
                out.append((self.part(step, z=moved("z", -d), r=rows), far, {"z": d}))
            return out
        name = axis_of(name)
        size = self.place.sizes[name]
        return [
            (self.part(step), self.part(step, **{name: moved(name, -d)}), {name: d}) for d in range(1, size)
        ]

    def made(self, step, came):
        slot = self.base
        for index in range(step):
            slot += len(self.copies(index))
        for source, landed, moves in self.copies(step):
            ref = landed if came else source
            yield remote(ref, ref, self.send.at[slot], self.recv.at[slot], self.place.device(**moves))
            slot += 1

    def start(self, step):
        for copy in self.made(step, False):
            copy.start()

    def arrive(self, step):
        for copy in self.made(step, True):
            copy.wait_recv()

    def next(self, step):
        if 0 < step <= len(self.steps):
            self.arrive(step - 1)
        if step < len(self.steps):
            self.start(step)

    def finish(self):
        for step in range(len(self.steps)):
            for copy in self.made(step, False):
                copy.wait_send()


def lanes(shape, limit):
    return lax.broadcasted_iota(jnp.int32, shape, 1) < limit


def token_rows(ref, seq, rows):
    return [ref[pl.ds(2 * j + seq, rows, stride=8), :] for j in range(4)]


def row_mean(parts):
    total = parts[0]
    for part in parts[1:]:
        total = total + part
    return jnp.sum(total, -1, keepdims=True) * (1.0 / (128 * len(parts)))


def normalize(parts):
    mean = row_mean(parts)
    center = [part - mean for part in parts]
    spread = row_mean([part * part for part in center])
    scale = lax.rsqrt(spread + 1e-05)
    return center, scale


def rope(value, cos, sin_a, sin_b):
    return value * cos + pltpu.roll(value, 96, 1) * sin_a + pltpu.roll(value, 32, 1) * sin_b


def rope_back(grad, cos, sin_a, sin_b):
    return grad * cos - pltpu.roll(grad, 96, 1) * sin_a - pltpu.roll(grad, 32, 1) * sin_b


def rope_tables(rows):
    half = HD // 2
    rates = np.exp(np.arange(half, dtype=np.float32) * np.float32(-2.0 * math.log(10000.0) / HD))
    angles = np.arange(rows, dtype=np.float32)[:, None] * rates.astype(np.float32)[None, :]
    cos, sin, zero = np.cos(angles), np.sin(angles), np.zeros_like(angles)
    tables = [[cos] * 4, [-sin, zero] * 2, [zero, sin] * 2]
    return jnp.asarray(np.stack([np.concatenate(table, -1) for table in tables]).astype(np.float32))


class Scatter:
    def __init__(self, place, view, work, order, dims, rows, lead, landing, final, send, recv, base):
        self.place, self.view, self.work, self.order, self.dims = place, view, work, order, dims
        self.lead, self.landing, self.final = lead, landing, final
        self.send, self.recv, self.base = send, recv, base
        self.low, self.high = pl.ds(0, rows // 2), pl.ds(rows // 2, rows // 2)
        self.steps = steps_of(place.sizes, order)
        self.order = order.lower()

    def done(self, step):
        return self.order[: self.order.index(axis_of(self.steps[step]))]

    def part(self, step, kept=False, **changed):
        where = dict(self.place.at)
        where["r"] = slice(None)
        for axis in self.order:
            if axis not in self.done(step):
                where[axis] = slice(None)
        where.update(changed)
        return (self.work if kept or step > 0 else self.view)(where)

    def sends(self, step):
        name, moved = self.steps[step], self.place.moved
        if name == "z1":
            return [({"z": moved("z", 2), "r": rows}, {"z": d}) for d, rows in ((1, self.low), (-1, self.high))]
        if name == "z2":
            return [({"z": moved("z", d)}, {"z": d}) for d in (1, -1)]
        name = axis_of(name)
        return [({name: moved(name, d)}, {name: d}) for d in range(1, self.place.sizes[name])]

    def sums(self, step):
        name, moved = self.steps[step], self.place.moved
        if name == "z1":
            return [({"z": moved("z", 1), "r": self.low}, [0]), ({"z": moved("z", -1), "r": self.high}, [1])]
        return [({axis_of(name): self.place.at[axis_of(name)]}, list(range(len(self.sends(step)))))]

    def made(self, step):
        slot = self.base
        for index in range(step):
            slot += len(self.sends(index))
        for index, (where, moves) in enumerate(self.sends(step)):
            yield remote(
                self.part(step, **where),
                self.landing[step].at[index],
                self.send.at[slot + index],
                self.recv.at[slot + index],
                self.place.device(**moves),
            )

    def start(self, step):
        for copy in self.made(step):
            copy.start()

    def arrive(self, step):
        for copy in self.made(step):
            copy.wait_recv()
        axis = axis_of(self.steps[step])
        rest = [a for a in self.dims if a in self.order and a not in self.done(step) and a != axis]
        sizes = [self.place.sizes[a] for a in rest]
        landing = self.landing[step]
        last = step == len(self.steps) - 1
        for where, pieces in self.sums(step):

            def add(index, carry, where=where, pieces=pieces):
                chosen = {}
                for a, size in zip(reversed(rest), reversed(sizes)):
                    chosen[a] = lax.rem(index, size)
                    index = index // size
                total = self.part(step, **chosen, **where)[...].astype(F32)
                for piece in pieces:
                    place = (piece,) + (slice(None),) * self.lead + tuple(chosen[a] for a in rest)
                    total = total + landing[place].astype(F32)
                if last:
                    self.final[...] = total
                else:
                    self.part(step, kept=True, **chosen, **where)[...] = total.astype(BF16)
                return carry

            count = math.prod(sizes)
            if count == 1:
                add(0, 0)
            else:
                lax.fori_loop(0, count, add, 0)

    def next(self, step):
        if 0 < step <= len(self.steps):
            self.arrive(step - 1)
        if step < len(self.steps):
            self.start(step)

    def finish(self):
        for step in range(len(self.steps)):
            for copy in self.made(step):
                copy.wait_send()


def landing_shapes(sizes, order, dims, rows, width, lead=(), lane_x=False):
    left = list(order.lower())
    shapes = []
    for step in steps_of(sizes, order):
        axis = axis_of(step)
        if step != "z2" and axis in left:
            left.remove(axis)
        count = 2 if step in ("z1", "z2") else sizes[axis] - 1
        high = rows // 2 if step == "z1" else rows
        wide = width * 2 if lane_x and "x" in left else width
        shapes.append((count,) + lead + tuple(sizes[a] for a in dims if a in left) + (high, wide))
    return shapes


def gelu_parts(value):
    cdf = 0.5 + 0.5 * lax.erf(value * (2.0**-0.5))
    density = jnp.exp(-0.5 * value * value) * ((2.0 * math.pi) ** -0.5)
    return value * cdf, cdf + value * density


GATHERS = (
    ("q", "Zyx"),
    ("k", "xyz"),
    ("v", "Zxy"),
    ("n", "zy"),
    ("out", "xyZc"),
    ("u0", "Zxyc"),
    ("u1", "Zxyc"),
    ("d0", "Zxyc"),
    ("d1", "xyzc"),
)
SCATTERS = (
    ("d0", "cZyx", "xczy", 256, False),
    ("d1", "cyZx", "xczy", 256, False),
    ("u0", "cxyZ", "xczy", 256, False),
    ("u1", "cyZx", "xczy", 256, False),
    ("out", "cxZy", "czy", 128, True),
    ("q", "yZx", "zy", 128, True),
    ("k", "yxZ", "zy", 128, True),
    ("v", "yZx", "zy", 128, True),
)
GATHER_AT = dict(
    f0=dict(q=(0,), k=(0,), v=(0,), out=(0,), u1=(0,), d1=(0,)),
    f1=dict(k=(1, 2,), n=(0,), u0=(0,)),
    f2=dict(q=(1,), v=(1,), u1=(1,), d1=(1,)),
    f3=dict(v=(2,)),
    f4=dict(q=(2,), k=(3,), out=(1,), d0=(0,)),
    f5=dict(n=(1,), u1=(2,)),
    f6=dict(u0=(1,), d1=(2,)),
    f7=dict(q=(3,), k=(4,), v=(3,)),
    m0=dict(n=(2,), out=(2,), d0=(1,)),
    b0=dict(u0=(2,)),
    m2=dict(u1=(3,)),
    b2=dict(d0=(2,)),
    m3=dict(d1=(3,)),
    b3=dict(out=(3,), u0=(3,)),
    e0=dict(n=(3,), out=(4,)),
    e1=dict(u0=(4,), u1=(4,), d0=(3,), d1=(4,)),
    e2=dict(d0=(4,), d1=(5,)),
)
SCATTER_AT = dict(
    g0=dict(d0=(0,)),
    g1=dict(u0=(0,), u1=(0,)),
    g2=dict(d0=(1,), u0=(1,), u1=(1,)),
    g3=dict(d1=(0, 1,)),
    g4=dict(out=(0, 1,)),
    n3=dict(u1=(2,)),
    n2=dict(u0=(2,)),
    t2=dict(d1=(2,)),
    t0=dict(out=(2,)),
    q0=dict(q=(0,)),
    q1=dict(u1=(3,)),
    q2=dict(u0=(3,), v=(0,)),
    q3=dict(k=(0,)),
    z0=dict(d0=(2,), q=(1,), v=(1,)),
    z1=dict(d1=(3,), out=(3,), k=(1,)),
    z2=dict(d0=(3,), u0=(4,), u1=(4,), q=(2,), k=(2,), v=(2, 3,)),
    z3=dict(d0=(4,), d1=(4,), out=(4,), q=(3,), k=(3,)),
)
HEADS = ("q", "k", "v")


def x_lane(index):
    return index if isinstance(index, slice) else pl.ds(pl.multiple_of(index * 128, 128), 128)


class Refs:
    pass


class Layer:
    def __init__(self, sizes, rows, tokens_total, refs):
        self.r = refs
        self.sizes, self.rows, self.own, self.tokens_total = sizes, rows, rows // 4, tokens_total
        self.place = Place(sizes)
        at = self.place.at
        self.x, self.c, self.z, self.y = at["x"], at["c"], at["z"], at["y"]
        self.t = self.x * 2 + self.c
        self.shard = 512 // (sizes["z"] * sizes["y"])
        self.half = lanes((self.own, 128), HD)
        self.zero = jnp.zeros((self.own, 128), BF16)
        self.gathers = self.make_gathers()
        self.scatters = self.make_scatters()
        self.sent = []

    def make_gathers(self):
        r = self.r

        def qkv_view(i):
            return lambda w: r.qkv_all.at[i, w["z"], w["y"], w["r"], x_lane(w["x"])]

        def ff_view(start):
            return lambda w: r.ff_all.at[w["x"], w["c"], w["z"], w["y"], w["r"], pl.ds(start, 256)]

        views = {
            "q": qkv_view(0),
            "k": qkv_view(1),
            "v": qkv_view(2),
            "n": lambda w: r.counts.at[w["z"], w["y"], w["r"]],
            "out": lambda w: r.out_all.at[w["c"], w["z"], w["y"], w["r"], x_lane(w["x"])],
            "u0": ff_view(0),
            "u1": ff_view(256),
            "d0": ff_view(512),
            "d1": ff_view(768),
        }
        plans, base = {}, 0
        for name, order in GATHERS:
            rows = 16 if name == "n" else self.shard
            plans[name] = Gather(self.place, views[name], order, rows, r.send_w, r.recv_w, base)
            base += slots_of(self.sizes, order)
        return plans

    def make_scatters(self):
        r = self.r

        def ff_view(start):
            return lambda w: r.grad_ff.at[w["x"], w["c"], w["z"], w["y"], w["r"], pl.ds(start, 256)]

        def ff_kept(start):
            return lambda w: r.ff_work.at[w["x"], w["z"], w["y"], w["r"], pl.ds(start, 256)]

        def qkv_view(i):
            return lambda w: r.grad_qkv.at[i, w["z"], w["y"], w["r"], x_lane(w["x"])]

        views = {
            "u0": (ff_view(0), ff_kept(0), r.up_final.at[:, pl.ds(0, 256)]),
            "u1": (ff_view(256), ff_kept(256), r.up_final.at[:, pl.ds(256, 256)]),
            "d0": (ff_view(512), ff_kept(512), r.down_final.at[:, pl.ds(0, 256)]),
            "d1": (ff_view(768), ff_kept(768), r.down_final.at[:, pl.ds(256, 256)]),
            "out": (
                lambda w: r.grad_out.at[w["c"], w["z"], w["y"], w["r"], x_lane(w["x"])],
                lambda w: r.out_work.at[w["z"], w["y"], w["r"], x_lane(w["x"])],
                r.out_final,
            ),
        }
        for i, name in enumerate("qkv"):
            views[name] = (qkv_view(i), qkv_view(i), r.qkv_final.at[i])
        plans, base, used = {}, 0, 0
        for name, order, dims, width, lane_x in SCATTERS:
            view, kept, final = views[name]
            count = len(steps_of(self.sizes, order))
            landing = r.landing[used : used + count]
            plans[name] = Scatter(
                self.place, view, kept, order, dims, self.shard, 0, landing, final, r.send_g, r.recv_g, base
            )
            used += count
            base += slots_of(self.sizes, order)
        return plans

    def point(self, label):
        for plans, places in ((self.gathers, GATHER_AT), (self.scatters, SCATTER_AT)):
            for name, steps in places.get(label, {}).items():
                for step in steps:
                    plans[name].next(step)

    def within(self, index, label):
        if label in GATHER_AT or label in SCATTER_AT:

            @pl.when(index)
            def _():
                self.point(label)

    def local(self, index, src, dst):
        copy = pltpu.make_async_copy(src, dst, self.r.local_sem.at[index])
        copy.start()
        return copy

    def row_block(self, index):
        return pl.ds(pl.multiple_of(index * self.own, self.own), self.own)

    def run(self):
        self.front()
        self.attention()
        self.feed_forward()
        self.attention_back()
        self.end()

    def front(self):
        r, place, x, c, own = self.r, self.place, self.x, self.c, self.own
        met = place.meet()
        copies = [
            self.local(0, r.qkv_shard, r.qkv_all.at[:, self.z, self.y, :, x_lane(x)]),
            self.local(1, r.out_shard, r.out_all.at[c, self.z, self.y, :, x_lane(x)]),
            self.local(2, r.up_shard, r.ff_all.at[x, c, self.z, self.y, :, pl.ds(0, 512)]),
            self.local(3, r.down_shard, r.ff_all.at[x, c, self.z, self.y, :, pl.ds(512, 512)]),
        ]
        load_x = self.local(4, r.x_hbm, r.x_ref)
        load_tables = self.local(5, r.tables_hbm, r.tables)
        self.loads = [self.local(6, r.teacher_hbm, r.teacher), self.local(7, r.cotangent_hbm, r.cotangent)]
        total = r.lengths[0] + r.lengths[1]
        r.counts[self.z, self.y] = jnp.full((16, 128), total.astype(F32))
        for copy in copies:
            copy.wait()
        met()
        self.point("f0")
        load_x.wait()
        for s in range(2):
            center, scale = normalize(token_rows(r.x_ref, s, own))
            for j in range(4):
                lane = pl.ds(128 * j, 128)
                value = center[j] * scale * r.gain_1[:, lane] + r.shift_1[:, lane]
                r.own_normed[s, :, lane] = value.astype(BF16)
        mine = self.row_block(self.t)

        def tokens(index, ref, moves):
            return remote(ref, ref, r.send_n.at[index], r.recv_n.at[index], place.device(**moves))

        sent = [
            remote(r.own_normed.at[1 - x], r.normed_all.at[mine], r.send_n.at[0], r.recv_n.at[0], place.device(x=1)),
            remote(r.own_normed.at[x], r.normed_all.at[mine], r.send_n.at[1], r.recv_n.at[1], place.device(c=1)),
        ]
        for copy in sent:
            copy.start()
        keep = self.local(0, r.own_normed.at[x], r.normed_all.at[mine])
        for label in ("f1", "f2", "f3"):
            self.point(label)
        far = r.normed_all.at[self.row_block((1 - x) * 2 + c)]
        tokens(0, far, {"x": 1}).wait_recv()
        sent.append(tokens(2, far, {"c": 1}))
        sent[-1].start()
        self.point("f4")
        self.point("f5")
        keep.wait()
        tokens(1, r.normed_all.at[self.row_block(x * 2 + 1 - c)], {"c": 1}).wait_recv()
        self.point("f6")
        tokens(2, r.normed_all.at[self.row_block((1 - x) * 2 + 1 - c)], {"c": 1}).wait_recv()
        self.point("f7")
        load_tables.wait()
        self.sent += sent

        w_qkv = [r.qkv_all[i].reshape(-1, 256) for i in range(3)]

        def project(index, carry):
            here = pl.ds(pl.multiple_of(index * own, own), own)
            normed = r.normed_all[here, :]
            cos, sin_a, sin_b = (r.tables[i, here, :] for i in range(3))
            for i, ref in ((0, r.q_all), (1, r.k_all), (2, r.v_all)):
                value = dot(normed, w_qkv[i])
                for pair in range(2):
                    lane = pl.ds(128 * pair, 128)
                    part = value[:, 128 * pair : 128 * pair + 128]
                    if i < 2:
                        part = rope(part, cos, sin_a, sin_b)
                    if i == 0:
                        part = part.astype(BF16) * jnp.asarray(HD**-0.5, BF16)
                    ref[here, lane] = part.astype(BF16)
            self.within(index == 1, "pr1")
            return carry

        lax.fori_loop(0, 4, project, 0)
        self.point("a")

    def hand(self, qb, act):
        r, t = self.r, self.t
        source, target = r.own_attended.at[pl.ds(qb * self.own, self.own)], r.attended.at[self.c, self.x]
        device = (lax.axis_index("dp"), jnp.asarray(qb, jnp.int32))

        @pl.when(t != qb)
        def _():
            copy = remote(source, target, r.send_a.at[qb], r.recv_a.at[t], device)
            copy.start() if act == "start" else copy.wait_send()

        if act == "start":

            @pl.when(t == qb)
            def _():
                pltpu.make_async_copy(source, target, r.recv_a.at[t]).start()

    def attention(self):
        r, own, half, zero = self.r, self.own, self.half, self.zero
        length = r.lengths[self.x]
        for qb in range(4):
            here = pl.ds(qb * own, own)
            keys = (qb + 1) * own
            key_pos = lax.broadcasted_iota(jnp.int32, (own, keys), 1)
            query_pos = lax.broadcasted_iota(jnp.int32, (own, keys), 0) + qb * own
            allowed = key_pos <= query_pos
            if qb > 1:
                allowed = allowed & (key_pos < length)

            def attend(pair, carry, qb=qb, here=here, keys=keys, allowed=allowed):
                lane = pl.ds(pl.multiple_of(pair * 128, 128), 128)
                queries = r.q_all[here, lane]
                k_part = r.k_all[pl.ds(0, keys), lane]
                v_part = r.v_all[pl.ds(0, keys), lane]
                mixed = []
                for head in range(2):
                    masked = jnp.where(half, queries, zero) if head == 0 else jnp.where(half, zero, queries)
                    scores = jnp.where(allowed, dot(masked, k_part, NT), -1e30)
                    highest = jnp.max(scores, -1, keepdims=True)
                    expd = jnp.exp(scores - highest)
                    denom = jnp.sum(expd, -1, keepdims=True)
                    probs = (expd * (1.0 / denom)).astype(BF16)
                    mixed.append(dot(probs, v_part))
                    wide = jnp.broadcast_to(highest + jnp.log(denom), (own, 128))
                    r.lse[pair * 2 + head, :, here] = jnp.transpose(wide)[:8]
                r.own_attended[here, lane] = jnp.where(half, mixed[0], mixed[1]).astype(BF16)
                self.within(pair == 0, "m%d" % qb)
                return carry

            lax.fori_loop(0, 2, attend, 0)
            self.hand(qb, "start")
            self.point("b%d" % qb)
        for pair in range(2):
            r.k_t[pair] = jnp.transpose(r.k_all[:, pl.ds(128 * pair, 128)])
        for k in range(2):
            for s in range(2):
                came = r.attended.at[k, s]
                remote(came, came, r.send_a.at[0], r.recv_a.at[s * 2 + k], self.place.device(x=1)).wait_recv()

    def feed_forward(self):
        r, own = self.r, self.own
        self.point("e0")
        count = jnp.sum(r.counts[...], axis=(0, 1))[0:1]
        factor = self.tokens_total / count
        weights = [r.out_all[k].reshape(512, 256) for k in range(2)]
        valid = []
        for s in range(2):
            rows = pl.ds(s * own, own)
            attn = dot(r.attended[0, s], weights[0], NT) + dot(r.attended[1, s], weights[1], NT)
            parts = token_rows(r.x_ref, s, own)
            for j in range(4):
                r.middle[rows, pl.ds(128 * j, 128)] = parts[j] + attn[:, 128 * j : 128 * j + 128]
            position = self.t * own + lax.broadcasted_iota(jnp.int32, (own, 128), 0)
            valid.append((position < r.lengths[s]).astype(F32))
        value = r.middle[...]
        mean = jnp.mean(value, -1, keepdims=True)
        center = value - mean
        scale = lax.rsqrt(jnp.mean(center * center, -1, keepdims=True) + 1e-05)
        normed = (center * scale * r.gain_2[...] + r.shift_2[...]).astype(BF16)
        normed_t = jnp.transpose(normed)

        def weight(t, start):
            return r.ff_all[t // 2, t % 2, :, :, :, pl.ds(start, 512)].reshape(512, 512)

        self.point("e1")

        def up(t, carry):
            act, slope = gelu_parts(dot(normed, weight(t, 0)))
            r.slope[t] = slope
            r.hidden[t] = act.astype(BF16)
            return carry

        lax.fori_loop(0, 4, up, 0)
        self.point("e2")
        r.total_sum[...] = jnp.zeros_like(r.total_sum)

        def down(t, carry):
            r.total_sum[...] += dot(r.hidden[t], weight(t, 512), NT)
            return carry

        lax.fori_loop(0, 4, down, 0)
        self.point("e3")
        for copy in self.loads:
            copy.wait()
        square = jnp.zeros((own, 128), F32)
        for s in range(2):
            rows = pl.ds(s * own, own)
            want = token_rows(r.teacher, s, own)
            pull = token_rows(r.cotangent, s, own)
            for j in range(4):
                lane = pl.ds(128 * j, 128)
                out = r.middle[rows, lane] + r.total_sum[rows, lane]
                r.output[pl.ds(2 * j + s, own, stride=8), :] = out
                differ = out - want[j]
                square = square + valid[s] * differ * differ
                r.seed[rows, lane] = factor * valid[s] * (pull[j] + differ)
        self.store = self.local(6, r.output, r.output_hbm)
        grad_f = r.seed[...].astype(BF16)
        grad_f_t = jnp.transpose(grad_f)
        r.total_sum[...] = jnp.zeros_like(r.total_sum)

        def put(t, start, value):
            value = value.astype(BF16).reshape(self.sizes["z"], self.sizes["y"], self.shard, 512)
            r.grad_ff[t // 2, t % 2, :, :, :, pl.ds(start, 512)] = value

        def back_down(t, carry):
            put(t, 512, dot(grad_f_t, r.hidden[t]))
            return carry

        lax.fori_loop(0, 4, back_down, 0)
        self.point("g0")

        def back_up(t, carry):
            grad_before = (r.slope[t] * dot(grad_f, weight(t, 512))).astype(BF16)
            put(t, 0, dot(normed_t, grad_before))
            r.total_sum[...] += dot(grad_before, weight(t, 0), NT)
            return carry

        lax.fori_loop(0, 4, back_up, 0)
        self.point("g1")
        grad_normed = r.total_sum[...]
        unit = (r.middle[...] - mean) * scale
        r.stat_send[0] = jnp.zeros_like(r.stat_send[0])
        r.stat_send[0, 0:1, 0:128] = jnp.sum(square, 0, keepdims=True)
        r.stat_send[0, 1:2] = jnp.sum(grad_normed * unit, 0, keepdims=True)
        r.stat_send[0, 2:3] = jnp.sum(grad_normed, 0, keepdims=True)
        scaled = grad_normed * r.gain_2[...]
        inner = jnp.mean(scaled * unit, -1, keepdims=True)
        grad = r.seed[...] + scale * (scaled - jnp.mean(scaled, -1, keepdims=True) - unit * inner)
        r.grad_middle[...] = grad
        branch = grad.astype(BF16)
        for k in range(2):
            grads = dot(branch, weights[k]).astype(BF16)
            for s in range(2):
                r.grad_attended[k, s] = grads[s * own : s * own + own]
        self.send_attended_back()
        self.point("g2")
        branch_t = jnp.transpose(branch)
        for k in range(2):
            value = dot(branch_t[:, :own], r.attended[k, 0]) + dot(branch_t[:, own:], r.attended[k, 1])
            r.grad_out[k] = value.astype(BF16).reshape(self.sizes["z"], self.sizes["y"], self.shard, 256)
        self.point("g3")

    def send_attended_back(self):
        r, at = self.r, self.place.at
        mine = r.g_all.at[self.row_block(self.t)]
        for index, moves in enumerate(({"x": 1}, {"x": 1, "c": 1}, {"c": 1})):
            to = dict(at)
            for axis in moves:
                to[axis] = 1 - at[axis]
            source = r.grad_attended.at[to["c"], to["x"]]
            copy = remote(source, mine, r.send_b.at[index], r.recv_b.at[self.t], self.place.device(**moves))
            copy.start()
            self.sent.append(copy)
        pltpu.make_async_copy(r.grad_attended.at[self.c, self.x], mine, r.recv_b.at[self.t]).start()

    def to_core(self, qb, act):
        r, i = self.r, qb // 2

        @pl.when(self.c != qb % 2)
        def _():
            source = r.grad_n.at[pl.ds(qb * self.own, self.own)]
            copy = remote(source, r.from_core.at[i], r.send_n.at[3 + i], r.recv_n.at[3 + i], self.place.device(c=1))
            copy.start() if act == "start" else copy.wait_send()

    def core_arrived(self, index):
        r = self.r
        slot = r.from_core.at[index]
        remote(slot, slot, r.send_n.at[3], r.recv_n.at[3 + index], self.place.device(c=1)).wait_recv()

    def cross(self):
        r = self.r
        return remote(r.to_x, r.from_x, r.send_n.at[5], r.recv_n.at[5], self.place.device(x=1))

    def to_chip(self, qb):
        r = self.r

        @pl.when((self.c == qb % 2) & (self.x != qb // 2))
        def _():
            self.core_arrived(qb // 2)
            r.to_x[...] = (r.grad_n[pl.ds(qb * self.own, self.own), :] + r.from_core[qb // 2]).astype(BF16)
            self.cross().start()

    def attention_back(self):
        r, own, half, zero = self.r, self.own, self.half, self.zero
        normed_t = jnp.transpose(r.normed_all[...])
        length = r.lengths[self.x]
        upper = lax.broadcasted_iota(jnp.int32, (128, own), 0) < HD
        w_qkv = [r.qkv_all[i].reshape(512, 256) for i in range(3)]
        self.point("g4")
        for qb in range(3, -1, -1):
            here = pl.ds(qb * own, own)
            keys = (qb + 1) * own
            seen = pl.ds(0, keys)
            key_pos = lax.broadcasted_iota(jnp.int32, (keys, own), 0)
            query_pos = lax.broadcasted_iota(jnp.int32, (keys, own), 1) + qb * own
            allowed = key_pos <= query_pos
            if qb > 1:
                allowed = allowed & (key_pos < length)
            came = r.g_all.at[here]
            remote(came, came, r.send_b.at[0], r.recv_b.at[qb], self.place.device(x=1)).wait_recv()

            def attend(pair, carry, qb=qb, here=here, seen=seen, allowed=allowed):
                lane = pl.ds(pl.multiple_of(pair * 128, 128), 128)
                queries = r.q_all[here, lane]
                grads = r.g_all[here, lane]
                k_part = r.k_all[seen, lane]
                v_part = r.v_all[seen, lane]
                dq = []
                for head in range(2):
                    if head == 0:
                        q_m, g_m = jnp.where(half, queries, zero), jnp.where(half, grads, zero)
                    else:
                        q_m, g_m = jnp.where(half, zero, queries), jnp.where(half, zero, grads)
                    scores = dot(k_part, q_m, NT)
                    probs = jnp.where(allowed, jnp.exp(scores - r.lse[pair * 2 + head, 0:1, here]), 0.0)
                    grad_probs = dot(v_part, g_m, NT)
                    inner = jnp.sum(probs * grad_probs, 0, keepdims=True)
                    grad_raw = (probs * (grad_probs - inner)).astype(BF16)
                    add_k = dot(grad_raw, q_m)
                    add_v = dot(probs.astype(BF16), g_m)
                    if qb == 3 and head == 0:
                        r.grad_k[seen, lane] = add_k
                        r.grad_v[seen, lane] = add_v
                    else:
                        r.grad_k[seen, lane] += add_k
                        r.grad_v[seen, lane] += add_v
                    dq.append(dot(r.k_t[pair, :, seen], grad_raw))
                r.grad_q[here, lane] = jnp.transpose(jnp.where(upper, dq[0], dq[1])) * HD**-0.5
                self.within(pair == 0, "n%d" % qb)
                return carry

            lax.fori_loop(0, 2, attend, 0)

            cos, sin_a, sin_b = (r.tables[i, here, :] for i in range(3))
            total = jnp.zeros((own, 512), F32)
            for i, ref in ((0, r.grad_q), (1, r.grad_k), (2, r.grad_v)):
                for pair in range(2):
                    lane = pl.ds(128 * pair, 128)
                    part = ref[here, lane]
                    if i < 2:
                        part = rope_back(part, cos, sin_a, sin_b)
                    r.grad_proj[i, here, lane] = part.astype(BF16)
                total = total + dot(r.grad_proj[i, here, :], w_qkv[i], NT)
            r.grad_n[here, :] = total
            self.to_core(qb, "start")
            if qb < 3:
                self.to_chip(qb + 1)
            self.point("t%d" % qb)
        for i, name in enumerate(HEADS):
            value = dot(normed_t, r.grad_proj[i]).astype(BF16)
            r.grad_qkv[i] = value.reshape(self.sizes["z"], self.sizes["y"], self.shard, 256)
            if i == 1:
                self.to_chip(0)
            self.point("q%d" % i)

    def end(self):
        r, own, x = self.r, self.own, self.x
        self.point("q3")
        self.core_arrived(x)
        self.cross().wait_recv()
        self.point("z0")
        grad_gain = [jnp.zeros((1, 128), F32)] * 4
        grad_shift = [jnp.zeros((1, 128), F32)] * 4
        for s in range(2):
            center, scale = normalize(token_rows(r.x_ref, s, own))
            near = r.grad_n[self.row_block(self.t), :] + r.from_core[x]
            chosen = jnp.where(x == s, near, r.from_x[...].astype(F32))
            grads = [chosen[:, 128 * j : 128 * j + 128] for j in range(4)]
            units = [part * scale for part in center]
            scaled = [grads[j] * r.gain_1[:, pl.ds(128 * j, 128)] for j in range(4)]
            mean = row_mean(scaled)
            inner = row_mean([scaled[j] * units[j] for j in range(4)])
            for j in range(4):
                part = r.grad_middle[pl.ds(s * own, own), pl.ds(128 * j, 128)]
                grad = part + scale * (scaled[j] - mean - units[j] * inner)
                r.grad_inputs[pl.ds(2 * j + s, own, stride=8), :] = grad
                grad_gain[j] = grad_gain[j] + jnp.sum(grads[j] * units[j], 0, keepdims=True)
                grad_shift[j] = grad_shift[j] + jnp.sum(grads[j], 0, keepdims=True)
        for j in range(4):
            r.stat_send[0, 3:4, 128 * j : 128 * j + 128] = grad_gain[j]
            r.stat_send[0, 4:5, 128 * j : 128 * j + 128] = grad_shift[j]
        slot = 0
        for phase, peers in enumerate((self.place.group(), self.place.across())):
            came = []
            for peer in peers:
                came.append(
                    remote(r.stat_send.at[phase], r.stat_land.at[slot], r.send_s.at[slot], r.recv_s.at[slot], peer)
                )
                came[-1].start()
                slot += 1
            self.point("z%d" % (phase + 1))
            total = r.stat_send[phase]
            for index, copy in enumerate(came):
                copy.wait_recv()
                total = total + r.stat_land[slot - len(came) + index]
            if phase == 0:
                r.stat_send[1] = total
            else:
                r.stats_final[...] = total
            self.sent += came
        self.point("z3")
        for plan in list(self.gathers.values()) + list(self.scatters.values()):
            plan.finish()
        for copy in self.sent + [self.cross()]:
            copy.wait_send()
        for qb in range(4):
            self.hand(qb, "finish")
            self.to_core(qb, "finish")
        self.store.wait()


def whole(sizes, rows, tokens_total, operands):
    zs, ys = sizes["z"], sizes["y"]
    shard = 512 // (zs * ys)
    own = rows // 4
    wide = own * 8
    inputs = dict(
        lengths=0, gain_1=0, shift_1=0, gain_2=0, shift_2=0, x_hbm=0,
        teacher_hbm=0, cotangent_hbm=0, tables_hbm=0, qkv_shard=0, out_shard=0, up_shard=0, down_shard=0,
    )
    outputs = dict(
        output_hbm=(wide, 128),
        grad_inputs=(wide, 128),
        up_final=(shard, 512),
        down_final=(shard, 512),
        out_final=(shard, 128),
        qkv_final=(3, shard, 128),
        stats_final=(8, 512),
        counts=(zs, ys, 16, 128),
    )
    scratch = dict(
        x_ref=((wide, 128), F32),
        teacher=((wide, 128), F32),
        cotangent=((wide, 128), F32),
        output=((wide, 128), F32),
        tables=((3, rows, 128), F32),
        ff_all=((2, 2, zs, ys, shard, 1024), BF16),
        out_all=((2, zs, ys, shard, 256), BF16),
        qkv_all=((3, zs, ys, shard, 256), BF16),
        own_normed=((2, own, 512), BF16),
        normed_all=((rows, 512), BF16),
        q_all=((rows, 256), BF16),
        k_all=((rows, 256), BF16),
        v_all=((rows, 256), BF16),
        k_t=((2, 128, rows), BF16),
        lse=((4, 8, rows), F32),
        own_attended=((rows, 256), BF16),
        attended=((2, 2, own, 256), BF16),
        middle=((2 * own, 512), F32),
        seed=((2 * own, 512), F32),
        slope=((4, 2 * own, 512), F32),
        hidden=((4, 2 * own, 512), BF16),
        total_sum=((2 * own, 512), F32),
        grad_middle=((2 * own, 512), F32),
        grad_attended=((2, 2, own, 256), BF16),
        grad_ff=((2, 2, zs, ys, shard, 1024), BF16),
        grad_out=((2, zs, ys, shard, 256), BF16),
        g_all=((rows, 256), BF16),
        grad_q=((rows, 256), F32),
        grad_k=((rows, 256), F32),
        grad_v=((rows, 256), F32),
        grad_proj=((3, rows, 256), BF16),
        grad_qkv=((3, zs, ys, shard, 256), BF16),
        grad_n=((rows, 512), F32),
        ff_work=((2, zs, ys, shard, 1024), BF16),
        out_work=((zs, ys, shard, 256), BF16),
        from_core=((2, own, 512), F32),
        to_x=((own, 512), BF16),
        from_x=((own, 512), BF16),
        stat_send=((2, 8, 512), F32),
        stat_land=((zs * ys + 2, 8, 512), F32),
    )
    gathered = sum(slots_of(sizes, order) for _, order in GATHERS)
    scattered = sum(slots_of(sizes, item[1]) for item in SCATTERS)
    sems = dict(local_sem=8, send_w=gathered, recv_w=gathered, send_g=scattered, recv_g=scattered)
    sems |= dict(send_n=6, recv_n=6, send_a=4, recv_a=4, send_b=3, recv_b=4)
    sems |= dict(send_s=zs * ys + 2, recv_s=zs * ys + 2)
    lands = []
    for _, order, dims, width, lane_x in SCATTERS:
        lands += landing_shapes(sizes, order, dims, shard, width, lane_x=lane_x)

    def kernel(*refs):
        refs = list(refs)
        out = Refs()
        for name in list(inputs) + list(outputs) + list(scratch) + list(sems):
            setattr(out, name, refs.pop(0))
        out.landing = refs
        Layer(sizes, rows, tokens_total, out).run()

    any_spec = pl.BlockSpec(memory_space=pl.ANY)
    vmem = pl.BlockSpec(memory_space=pltpu.VMEM)
    return pl.pallas_call(
        kernel,
        out_shape=[jax.ShapeDtypeStruct(shape, F32) for shape in outputs.values()],
        in_specs=[pl.BlockSpec(memory_space=pltpu.SMEM)] + [vmem] * 4 + [any_spec] * 8,
        out_specs=[any_spec] + [vmem] * (len(outputs) - 1),
        scratch_shapes=[pltpu.VMEM(*shape) for shape in scratch.values()]
        + [pltpu.SemaphoreType.DMA((count,)) for count in sems.values()]
        + [pltpu.VMEM(shape, BF16) for shape in lands],
        name="whole",
        compiler_params=pltpu.CompilerParams(
            collective_id=0, has_side_effects=True, vmem_limit_bytes=VMEM_LIMIT
        ),
    )(*operands)


def last_kernel(features, counts, output, grad_inputs, up, down, out, qkv, sums, *outs):
    for source, target in zip((output, grad_inputs, up, down, out, qkv), outs[:6]):
        target[...] = source[...]
    for target, row in zip(outs[6:10], (3, 4, 1, 2)):
        target[...] = sums[row : row + 1]
    total = jnp.sum(counts[...], axis=0)[0:1, 0:1]
    outs[10][...] = jnp.sum(sums[0:1, 0:128], -1, keepdims=True) / (total * features)


def last(features, counts, output, grad_inputs, up, down, out, qkv, sums):
    vmem = pl.BlockSpec(memory_space=pltpu.VMEM)
    shapes = [value.shape for value in (output, grad_inputs, up, down, out, qkv)] + [(1, features)] * 4 + [(1, 1)]
    return pl.pallas_call(
        lambda *refs: last_kernel(features, *refs),
        out_shape=[jax.ShapeDtypeStruct(shape, F32) for shape in shapes],
        in_specs=[vmem] * 8,
        out_specs=[vmem] * len(shapes),
        name="last",
        compiler_params=pltpu.CompilerParams(vmem_limit_bytes=VMEM_LIMIT),
    )(counts, output, grad_inputs, up, down, out, qkv, sums)


def solution(mesh):
    dp, tensor = mesh.shape["dp"], mesh.shape["tensor"]
    sizes = {"z": dp // 2, "y": 2, "x": tensor // 2, "c": 2}

    def shards(
        inputs, qkv_weight, out_weight, up_weight, down_weight, gain_one, shift_one, gain_two, shift_two, lengths,
        teacher, cotangent,
    ):
        own, sequences, width = inputs.shape
        rows = own * tensor

        def packed(value):
            view = value.reshape(own, sequences, width // 128, 128).transpose(0, 2, 1, 3)
            return view.reshape(own * sequences * (width // 128), 128)

        def unpacked(value):
            view = value.reshape(own, width // 128, sequences, 128).transpose(0, 2, 1, 3)
            return view.reshape(own, sequences, width)

        operands = (
            lengths, gain_one[None], shift_one[None], gain_two[None], shift_two[None], packed(inputs), packed(teacher),
            packed(cotangent), rope_tables(rows), qkv_weight, out_weight.T, up_weight, down_weight.T,
        )
        *parts, sums, counts = whole(sizes, rows, float(rows * sequences * dp), operands)
        output, grad_inputs, up, down, out, qkv, gain_1, shift_1, gain_2, shift_2, loss = last(
            width, counts.reshape(dp, 16, 128), *parts, sums
        )
        return (
            unpacked(output), loss.reshape(()), unpacked(grad_inputs), qkv, out.T, up, down.T, gain_1.reshape(width),
            shift_1.reshape(width), gain_2.reshape(width), shift_2.reshape(width),
        )

    tokens, rows_dp, cols_dp = P("tensor", "dp", None), P("dp", "tensor"), P("tensor", "dp")
    heads = P(None, "dp", "tensor")
    return jax.shard_map(
        shards,
        mesh=mesh,
        in_specs=(tokens, heads, cols_dp, rows_dp, cols_dp, P(), P(), P(), P(), P("dp"), tokens, tokens),
        out_specs=(tokens, P(), tokens, heads, cols_dp, rows_dp, cols_dp, P(), P(), P(), P()),
        check_vma=False,
    )
```
